32 devices in a mesh: gx: 16 (over z, y, x), gy: 2 (over core).
Axes of the slice: x: 2, y: 2, z: 4, core: 2. Of those that a mesh axis runs over, the one named last changes fastest.
Arguments:
- fields: float32 [5, 192, 32, 128], P(None, 'gx', 'gy'), may hold values from -1.5 to 6, as said below
- phase_map: int32 [192, 32, 128], P('gx', 'gy'), may hold values from 0 to 1, as said below
- lagged_speed: float32 [1], replicated, may hold values from 7 to 17, as said below
- step_count: int32 [1], replicated, may hold values from 0 to 1023
Outputs:
- advanced: float32 [5, 192, 32, 128], P(None, 'gx', 'gy')
- next_speed: float32 [1], replicated
The draws below stay inside these ranges and needn't reach their ends.
Inputs may be any that keep to these rules, and one draw needn't show every extreme that they name: `phase_map`: in each column (fixed first and second index) the cells below a level between 32 and 96, drawn per column, are 1 and the cells above it are 0. Density lies within 1 to 2 in cells of phase 0 and within 1 to 4 in cells of phase 1; the pressure P(fields) lies within 0.6 to 1.6 and every velocity m_k / rho within -0.3 to 0.3. lagged_speed[0] lies between 1.01 and 1.31 times the largest over all cells of fields of |v_1| + |v_2| + |v_3| + 3 sqrt(gamma_cell (P + pinf_cell) / rho).
All inputs are finite; a program needn't handle non-finite values.
Results may differ from the reference program's by a relative error of at most 0.00002.
Values sent between devices are 32-bit elements; how exact they have to be, the bound alone decides.
No kernel may reach another device: no remote copies, remote signals or barrier semaphores. Data moves between devices by JAX's collectives and lax.ppermute only.
A program may use at most 128 MiB of HBM per device.

```python
import math
import jax
import jax.numpy as jnp

PERIOD = 64
NX = 192
NY = 32
NZ = 128


def column_phase(key):
    levels = jax.random.randint(jax.random.fold_in(key, 11), (NX, NY, 1), NZ // 4, 3 * NZ // 4 + 1)
    height = jnp.arange(NZ, dtype=jnp.int32).reshape(1, 1, NZ)
    return (height < levels).astype(jnp.int32)


def drawn_state(key):
    water_frac = column_phase(key).astype(jnp.float32)
    subkeys = jax.random.split(jax.random.fold_in(key, 12), 5)
    grid_shape = (NX, NY, NZ)
    first_hot = jax.random.randint(subkeys[3], (), 0, NX)
    offset = (jnp.arange(NX, dtype=jnp.int32) - first_hot) % NX
    inside = (offset < max(NX // 32, 1)).astype(jnp.float32).reshape(NX, 1, 1)
    heat = 1.05 + 0.1 * jax.random.uniform(subkeys[4], ())
    water_level = 2.0 / (1.0 + inside * (heat * heat - 1.0))
    density = (1.0 + jax.random.uniform(subkeys[0], grid_shape)) * (1.0 + water_frac * (water_level - 1.0))
    press_now = 0.6 + jax.random.uniform(subkeys[1], grid_shape)
    velocity = 0.3 * jax.random.uniform(subkeys[2], (3,) + grid_shape, minval=-1.0, maxval=1.0)
    return (water_frac, density, press_now, velocity)


def draw_phase_map(key, part):
    return column_phase(key)


def draw_fields(key, part):
    water_frac, density, press_now, velocity = drawn_state(key)
    gamma_cell = 1.4 + 3.0 * water_frac
    pinf_cell = 3.0 * water_frac
    kinetic = 0.5 * density * jnp.sum(velocity * velocity, axis=0)
    energy = (press_now + gamma_cell * pinf_cell) / (gamma_cell - 1.0) + kinetic
    momentum = density * velocity
    return jnp.stack([density, momentum[0], momentum[1], momentum[2], energy])


def draw_lagged_speed(key, part):
    water_frac, density, press_now, velocity = drawn_state(key)
    gamma_cell = 1.4 + 3.0 * water_frac
    pinf_cell = 3.0 * water_frac
    speed = jnp.sum(jnp.abs(velocity), axis=0) + 3.0 * jnp.sqrt(gamma_cell * (press_now + pinf_cell) / density)
    margin = 1.01 + 0.3 * jax.random.uniform(jax.random.fold_in(key, 13), ())
    return jnp.reshape(jnp.max(speed) * margin, (1,))


def setup_inputs(seed: int = 0) -> dict:
    arg_keys = jax.random.split(jax.random.key(seed), 5)
    fields = draw_fields(jax.random.fold_in(arg_keys[4], 71), 0)
    phase_map = draw_phase_map(jax.random.fold_in(arg_keys[4], 71), 0)
    lagged_speed = draw_lagged_speed(jax.random.fold_in(arg_keys[4], 71), 0)
    step_count = jax.random.randint(arg_keys[3], (1,), 0, 16 * PERIOD).astype(jnp.int32)
    return {"fields": fields, "phase_map": phase_map, "lagged_speed": lagged_speed, "step_count": step_count}


gamma_air = 1.4
gamma_water = 4.4
pinf_water = 3.0
cfl_number = 0.9
gravity = 1.0
shake_amp = 0.8
two_pi = 2.0 * math.pi
coef_one = 0.75
coef_two = -0.15
coef_three = 1.0 / 60.0
one_third = 1.0 / 3.0
two_thirds = 2.0 / 3.0

def pressure(fields, gamma_cell, pinf_cell):
    inverse = 1.0 / fields[0]
    kinetic = 0.5 * (fields[1] * (fields[1] * inverse) + fields[2] * (fields[2] * inverse) + fields[3] * (fields[3] * inverse))
    return (gamma_cell - 1.0) * (fields[4] - kinetic) - gamma_cell * pinf_cell

def fluxes(fields, press_now, direction):
    inverse = 1.0 / fields[0]
    velocity = fields[1 + direction] * inverse
    pieces = [fields[1 + direction]]
    for member in range(3):
        moment = fields[1 + member] * velocity
        if member == direction:
            moment = moment + press_now
        pieces.append(moment)
    pieces.append((fields[4] + press_now) * velocity)
    return jnp.stack(pieces)

def roll_one(values, along):

    def shifted(offset):
        return jnp.roll(values, -offset, along)
    return coef_one * (shifted(1) - shifted(-1)) + coef_two * (shifted(2) - shifted(-2)) + coef_three * (shifted(3) - shifted(-3))

def slope_roll(values, along):
    return jnp.stack([roll_one(values[member], along - 1) for member in range(values.shape[0])])

def sources(fields, gravity_now):
    blank = jnp.zeros_like(fields[0])
    return jnp.stack([blank, blank, blank, fields[0] * gravity_now, fields[3] * gravity_now])

def section_rates(fields, gamma_cell, pinf_cell, gravity_now):
    press_now = pressure(fields, gamma_cell, pinf_cell)
    divergence = slope_roll(fluxes(fields, press_now, 0), 1) + slope_roll(fluxes(fields, press_now, 1), 2)
    divergence = divergence + slope_roll(fluxes(fields, press_now, 2), 3)
    return sources(fields, gravity_now) - divergence

def top_speed(fields, gamma_cell, pinf_cell):
    press_now = pressure(fields, gamma_cell, pinf_cell)
    inverse = 1.0 / fields[0]
    local_speed = jnp.abs(fields[1] * inverse) + jnp.abs(fields[2] * inverse) + jnp.abs(fields[3] * inverse)
    local_speed = local_speed + 3.0 * jnp.sqrt(gamma_cell * (press_now + pinf_cell) * inverse)
    return jnp.max(local_speed)

def reference(fields, phase_map, lagged_speed, step_count):
    water_frac = phase_map.astype(jnp.float32)
    gamma_cell = gamma_air + (gamma_water - gamma_air) * water_frac
    pinf_cell = pinf_water * water_frac
    time_step = cfl_number / lagged_speed[0]
    gravity_now = gravity * (1.0 + shake_amp * jnp.cos(two_pi * step_count[0].astype(jnp.float32) / PERIOD))
    section_one = fields + time_step * section_rates(fields, gamma_cell, pinf_cell, gravity_now)
    section_two = 0.75 * fields + 0.25 * (section_one + time_step * section_rates(section_one, gamma_cell, pinf_cell, gravity_now))
    advanced = one_third * fields + two_thirds * (section_two + time_step * section_rates(section_two, gamma_cell, pinf_cell, gravity_now))
    return (advanced, jnp.reshape(top_speed(advanced, gamma_cell, pinf_cell), (1,)))
```

```python
import math

import jax
import jax.numpy as jnp
from jax import lax
from jax.sharding import PartitionSpec as P

PERIOD = 64


gamma_air = 1.4
gamma_water = 4.4
pinf_water = 3.0
cfl_number = 0.9
gravity = 1.0
shake_amp = 0.8
two_pi = 2.0 * math.pi
coef_one = 0.75
coef_two = -0.15
coef_three = 1.0 / 60.0
one_third = 1.0 / 3.0
two_thirds = 2.0 / 3.0


def padded(array, sides, width):
    for axis, dim in sides:
        count, length = (lax.axis_size(axis), array.shape[dim])
        up = [(i, (i + 1) % count) for i in range(count)]
        down = [(j, i) for i, j in up]
        last = lax.slice_in_dim(array, length - width, length, axis=dim)
        leading = lax.slice_in_dim(array, 0, width, axis=dim)
        before = lax.ppermute(last, axis, up)
        after = lax.ppermute(leading, axis, down)
        array = jnp.concatenate([before, array, after], axis=dim)
    return array


def pressure(fields, gamma_cell, pinf_cell):
    inverse = 1.0 / fields[0]
    kinetic = 0.5 * (
        fields[1] * (fields[1] * inverse)
        + fields[2] * (fields[2] * inverse)
        + fields[3] * (fields[3] * inverse)
    )
    return (gamma_cell - 1.0) * (fields[4] - kinetic) - gamma_cell * pinf_cell


def fluxes(fields, press_now, direction):
    inverse = 1.0 / fields[0]
    velocity = fields[1 + direction] * inverse
    pieces = [fields[1 + direction]]
    for member in range(3):
        moment = fields[1 + member] * velocity
        if member == direction:
            moment = moment + press_now
        pieces.append(moment)
    pieces.append((fields[4] + press_now) * velocity)
    return jnp.stack(pieces)


def roll_one(values, along):

    def shifted(offset):
        return jnp.roll(values, -offset, along)

    return (
        coef_one * (shifted(1) - shifted(-1))
        + coef_two * (shifted(2) - shifted(-2))
        + coef_three * (shifted(3) - shifted(-3))
    )


def slope_roll(values, along):
    return jnp.stack([roll_one(values[member], along - 1) for member in range(values.shape[0])])


def slide_along(values, along):
    length = values.shape[along] - 6

    def window(offset):
        return lax.slice_in_dim(values, 3 + offset, 3 + offset + length, axis=along)

    return (
        coef_one * (window(1) - window(-1))
        + coef_two * (window(2) - window(-2))
        + coef_three * (window(3) - window(-3))
    )


def sources(fields, gravity_now):
    blank = jnp.zeros_like(fields[0])
    return jnp.stack([blank, blank, blank, fields[0] * gravity_now, fields[3] * gravity_now])


def local(fields, phase_map, lagged_speed, step_count):
    water_frac = phase_map.astype(jnp.float32)
    gamma_cell = gamma_air + (gamma_water - gamma_air) * water_frac
    pinf_cell = pinf_water * water_frac
    time_step = cfl_number / lagged_speed[0]
    gravity_now = gravity * (
        1.0 + shake_amp * jnp.cos(two_pi * step_count[0].astype(jnp.float32) / PERIOD)
    )

    def section_rates(state, gamma_here, pinf_here):
        press_now = pressure(state, gamma_here, pinf_here)
        along_first = fluxes(state, press_now, 0)
        along_second = fluxes(state, press_now, 1)
        wide_first = padded(along_first, (("gx", 1),), 3)
        wide_second = padded(along_second, (("gy", 2),), 3)
        divergence = slide_along(wide_first, 1) + slide_along(wide_second, 2)
        divergence = divergence + slope_roll(fluxes(state, press_now, 2), 3)
        return sources(state, gravity_now) - divergence

    section_one = fields + time_step * section_rates(fields, gamma_cell, pinf_cell)
    section_two = 0.75 * fields + 0.25 * (
        section_one + time_step * section_rates(section_one, gamma_cell, pinf_cell)
    )
    advanced = one_third * fields + two_thirds * (
        section_two + time_step * section_rates(section_two, gamma_cell, pinf_cell)
    )
    press_now = pressure(advanced, gamma_cell, pinf_cell)
    inverse = 1.0 / advanced[0]
    local_speed = (
        jnp.abs(advanced[1] * inverse)
        + jnp.abs(advanced[2] * inverse)
        + jnp.abs(advanced[3] * inverse)
    )
    local_speed = local_speed + 3.0 * jnp.sqrt(gamma_cell * (press_now + pinf_cell) * inverse)
    members = lax.axis_size("gx") * lax.axis_size("gy")
    copies = jnp.broadcast_to(jnp.max(local_speed), (members,))
    largest = jnp.max(lax.all_to_all(copies, ("gx", "gy"), 0, 0, tiled=True))
    return (advanced, jnp.reshape(largest, (1,)))


def solution(mesh):
    return jax.shard_map(
        local,
        mesh=mesh,
        in_specs=(P(None, "gx", "gy", None), P("gx", "gy", None), P(), P()),
        out_specs=(P(None, "gx", "gy", None), P()),
        check_vma=False,
    )
```

```python
import functools
import math

import jax
import jax.numpy as jnp
from jax import lax
from jax.experimental import pallas as pl
from jax.experimental.pallas import tpu as pltpu
from jax.sharding import PartitionSpec as P

PERIOD = 64


gamma_air = 1.4
gamma_water = 4.4
pinf_water = 3.0
cfl_number = 0.9
gravity = 1.0
shake_amp = 0.8
two_pi = 2.0 * math.pi
coef_one = 0.75
coef_two = -0.15
coef_three = 1.0 / 60.0
one_third = 1.0 / 3.0
two_thirds = 2.0 / 3.0

WIDTH = 3
TILE = 8
VMEM = pl.BlockSpec(memory_space=pltpu.VMEM)
SMEM = pl.BlockSpec(memory_space=pltpu.SMEM)


def point(state, phase):
    density, one, two, three, energy = state
    water_frac = phase.astype(jnp.float32)
    gamma_cell = gamma_air + (gamma_water - gamma_air) * water_frac
    pinf_cell = pinf_water * water_frac
    inverse = 1.0 / density
    velocity = (one * inverse, two * inverse, three * inverse)
    kinetic = 0.5 * (one * velocity[0] + two * velocity[1] + three * velocity[2])
    press_now = (gamma_cell - 1.0) * (energy - kinetic) - gamma_cell * pinf_cell
    return velocity, press_now, inverse, gamma_cell, pinf_cell


def flux(state, velocity, press_now, direction):
    speed = velocity[direction]
    pieces = [state[1 + direction]]
    for member in range(3):
        moment = state[1 + member] * speed
        pieces.append(moment + press_now if member == direction else moment)
    pieces.append((state[4] + press_now) * speed)
    return pieces


def plane(ref, index):
    return [ref[member, index] for member in range(5)]


def edge_fluxes(state_ref, phase_ref, last_ref, leading_ref):
    length = state_ref.shape[1]
    for target, start in ((last_ref, length - WIDTH), (leading_ref, 0)):
        for k in range(WIDTH):
            state = plane(state_ref, start + k)
            velocity, press_now, *_ = point(state, phase_ref[start + k])
            for member, piece in enumerate(flux(state, velocity, press_now, 0)):
                target[member, k] = piece


def edge_kernel(state_ref, phase_ref, last_ref, leading_ref):
    edge_fluxes(state_ref, phase_ref, last_ref, leading_ref)


def rows_kernel(state_ref, phase_ref, rows_ref):
    rows = state_ref.shape[2]
    below = lax.broadcasted_iota(jnp.int32, (TILE, state_ref.shape[3]), 0) < TILE // 2

    def body(index, carry):
        state = []
        for member in range(5):
            first = state_ref[member, index, 0:TILE]
            final = state_ref[member, index, rows - TILE : rows]
            state.append(jnp.where(below, first, final))
        phase = jnp.where(below, phase_ref[index, 0:TILE], phase_ref[index, rows - TILE : rows])
        velocity, press_now, *_ = point(state, phase)
        for member, piece in enumerate(flux(state, velocity, press_now, 1)):
            rows_ref[member, index] = piece
        return carry

    lax.fori_loop(0, state_ref.shape[1], body, 0, unroll=2)


def middle_kernel(weights, first, coefs, state_ref, phase_ref, start_ref, before_ref, after_ref, out_ref, xs, ys, zs):
    length, rows, lanes = phase_ref.shape
    blank = jnp.zeros((rows, lanes), jnp.float32)
    for member in range(5):
        for k in range(WIDTH):
            xs[member, k] = blank
            xs[member, WIDTH + length + k] = blank

    def fill(index, carry):
        state = plane(state_ref, index)
        velocity, press_now, *_ = point(state, phase_ref[index])
        for member, piece in enumerate(flux(state, velocity, press_now, 0)):
            xs[member, WIDTH + index] = piece
        for member, piece in enumerate(flux(state, velocity, press_now, 1)):
            ys[member, index, TILE : TILE + rows] = piece
            ys[member, index, 0:TILE] = before_ref[member, index]
            ys[member, index, TILE + rows : TILE + rows + TILE] = after_ref[member, index]
        for member, piece in enumerate(flux(state, velocity, press_now, 2)):
            zs[member, index] = piece
        return carry

    lax.fori_loop(0, length, fill, 0, unroll=2)
    keep, share = weights
    steps = [coefs[k] * share for k in range(3)]
    source = coefs[3] * share

    def update(index, carry):
        for member in range(5):
            third = zs[member, index]
            total = None
            for k in range(1, WIDTH + 1):
                ahead = xs[member, WIDTH + index + k] - xs[member, WIDTH + index - k]
                ahead = ahead + (
                    ys[member, index, TILE + k : TILE + k + rows] - ys[member, index, TILE - k : TILE - k + rows]
                )
                ahead = ahead + (pltpu.roll(third, lanes - k, 1) - pltpu.roll(third, k, 1))
                term = steps[k - 1] * ahead
                total = term if total is None else total + term
            value = state_ref[member, index]
            if first:
                value = value - total
            else:
                value = keep * start_ref[member, index] + (share * value - total)
            if member == 3:
                value = value + source * state_ref[0, index]
            if member == 4:
                value = value + source * state_ref[3, index]
            out_ref[member, index] = value
        return carry

    lax.fori_loop(0, length, update, 0)


def add_halo(share, coefs, partial_ref, left_ref, right_ref, out_ref):
    length = partial_ref.shape[1]
    steps = [coefs[k] * share for k in range(3)]
    for member in range(5):
        for near in range(WIDTH):
            left = partial_ref[member, near]
            right = partial_ref[member, length - 1 - near]
            for k in range(near + 1, WIDTH + 1):
                left = left + steps[k - 1] * left_ref[member, WIDTH + near - k]
                right = right - steps[k - 1] * right_ref[member, k - 1 - near]
            out_ref[member, near] = left
            out_ref[member, length - 1 - near] = right


def join_kernel(share, coefs, partial_ref, left_ref, right_ref, phase_ref, out_ref, last_ref, leading_ref):
    add_halo(share, coefs, partial_ref, left_ref, right_ref, out_ref)
    edge_fluxes(out_ref, phase_ref, last_ref, leading_ref)


def final_kernel(share, coefs, partial_ref, left_ref, right_ref, phase_ref, out_ref, peak_ref):
    length, rows, lanes = phase_ref.shape
    add_halo(share, coefs, partial_ref, left_ref, right_ref, out_ref)
    for index in range(WIDTH, length - WIDTH):
        for member in range(5):
            out_ref[member, index] = partial_ref[member, index]

    def body(index, largest):
        state = plane(out_ref, index)
        velocity, press_now, inverse, gamma_cell, pinf_cell = point(state, phase_ref[index])
        speed = jnp.abs(velocity[0]) + jnp.abs(velocity[1]) + jnp.abs(velocity[2])
        speed = speed + 3.0 * jnp.sqrt(gamma_cell * (press_now + pinf_cell) * inverse)
        return jnp.maximum(largest, speed)

    largest = lax.fori_loop(0, length, body, jnp.zeros((rows, lanes), jnp.float32), unroll=2)
    largest = jnp.max(largest, axis=0, keepdims=True)
    peak_ref[...] = jnp.broadcast_to(largest, peak_ref.shape)


def peak_kernel(peaks_ref, largest_ref):
    largest = jnp.max(jnp.max(peaks_ref[...], axis=0, keepdims=True), axis=1, keepdims=True)
    largest_ref[...] = largest


def shaped(*shape):
    return jax.ShapeDtypeStruct(shape, jnp.float32)


def call(kernel, outs, specs, args, *, flops, scratch=(), aliases=None):
    moved = 4 * sum(math.prod(o.shape) for o in outs)
    several = len(outs) > 1
    return pl.pallas_call(
        kernel,
        out_shape=list(outs) if several else outs[0],
        in_specs=specs,
        out_specs=[VMEM] * len(outs) if several else VMEM,
        scratch_shapes=list(scratch),
        input_output_aliases=aliases or {},
        cost_estimate=pl.CostEstimate(flops=flops, bytes_accessed=moved, transcendentals=0),
        compiler_params=pltpu.CompilerParams(vmem_limit_bytes=16 << 20),
    )(*args)


def local(fields, phase_map, lagged_speed, step_count):
    _, length, rows, lanes = fields.shape
    cells = length * rows * lanes
    time_step = cfl_number / lagged_speed[0]
    gravity_now = gravity * (
        1.0 + shake_amp * jnp.cos(two_pi * step_count[0].astype(jnp.float32) / PERIOD)
    )
    coefs = time_step * jnp.stack(
        [jnp.float32(coef_one), jnp.float32(coef_two), jnp.float32(coef_three), gravity_now]
    )
    along, across = lax.axis_size("gx"), lax.axis_size("gy")
    up = [(i, (i + 1) % along) for i in range(along)]
    down = [(j, i) for i, j in up]
    over = [(i, (i + 1) % across) for i in range(across)]
    back = [(j, i) for i, j in over]
    edge = shaped(5, WIDTH, rows, lanes)
    whole = shaped(5, length, rows, lanes)
    row_tile = shaped(5, length, TILE, lanes)

    state = fields
    last, leading = call(
        edge_kernel, [edge, edge], [VMEM, VMEM], [state, phase_map], flops=cells * 20
    )
    stages = ((0.0, 1.0), (0.75, 0.25), (one_third, two_thirds))
    for number, weights in enumerate(stages):
        left = lax.ppermute(last, "gx", up)
        right = lax.ppermute(leading, "gx", down)
        sent = call(rows_kernel, [row_tile], [VMEM, VMEM], [state, phase_map], flops=cells * 10)
        before = lax.ppermute(sent, "gy", over)
        after = before if across == 2 else lax.ppermute(sent, "gy", back)
        partial = call(
            functools.partial(middle_kernel, weights, number == 0),
            [whole],
            [SMEM] + [VMEM] * 5,
            [coefs, state, phase_map, fields, before, after],
            flops=cells * 2000,
            scratch=[
                pltpu.VMEM((5, length + 2 * WIDTH, rows, lanes), jnp.float32),
                pltpu.VMEM((5, length, rows + 2 * TILE, lanes), jnp.float32),
                pltpu.VMEM((5, length, rows, lanes), jnp.float32),
            ],
        )
        if number < 2:
            state, last, leading = call(
                functools.partial(join_kernel, weights[1]),
                [whole, edge, edge],
                [SMEM] + [VMEM] * 4,
                [coefs, partial, left, right, phase_map],
                flops=cells * 20,
                aliases={1: 0},
            )
        else:
            advanced, peak = call(
                functools.partial(final_kernel, weights[1]),
                [whole, shaped(along * across, lanes)],
                [SMEM] + [VMEM] * 4,
                [coefs, partial, left, right, phase_map],
                flops=cells * 50,
            )
    peaks = lax.all_to_all(peak, ("gx", "gy"), 0, 0, tiled=True)
    largest = call(peak_kernel, [shaped(1, 1)], [VMEM], [peaks], flops=1000)
    return (advanced, jnp.reshape(largest, (1,)))


def solution(mesh):
    return jax.shard_map(
        local,
        mesh=mesh,
        in_specs=(P(None, "gx", "gy", None), P("gx", "gy", None), P(), P()),
        out_specs=(P(None, "gx", "gy", None), P()),
        check_vma=False,
    )
```

```python
import functools
import math

import jax
import jax.numpy as jnp
from jax import lax
from jax.experimental import pallas as pl
from jax.experimental.pallas import tpu as pltpu
from jax.sharding import PartitionSpec as P


PERIOD = 64


gamma_air = 1.4
gamma_water = 4.4
pinf_water = 3.0
cfl_number = 0.9
gravity = 1.0
shake_amp = 0.8
two_pi = 2.0 * math.pi
coef_one = 0.75
coef_two = -0.15
coef_three = 1.0 / 60.0
one_third = 1.0 / 3.0
two_thirds = 2.0 / 3.0

WIDTH = 3
TILE = 8
VMEM = pl.BlockSpec(memory_space=pltpu.VMEM)
SMEM = pl.BlockSpec(memory_space=pltpu.SMEM)
HBM = pl.BlockSpec(memory_space=pltpu.HBM)


def point(state, phase):
    density, one, two, three, energy = state
    water_frac = phase.astype(jnp.float32)
    gamma_cell = gamma_air + (gamma_water - gamma_air) * water_frac
    pinf_cell = pinf_water * water_frac
    inverse = 1.0 / density
    velocity = (one * inverse, two * inverse, three * inverse)
    kinetic = 0.5 * (one * velocity[0] + two * velocity[1] + three * velocity[2])
    press_now = (gamma_cell - 1.0) * (energy - kinetic) - gamma_cell * pinf_cell
    return velocity, press_now, inverse, gamma_cell, pinf_cell


def flux(state, velocity, press_now, direction):
    speed = velocity[direction]
    pieces = [state[1 + direction]]
    for member in range(3):
        moment = state[1 + member] * speed
        pieces.append(moment + press_now if member == direction else moment)
    pieces.append((state[4] + press_now) * speed)
    return pieces


def plane(ref, index):
    return [ref[member, index] for member in range(5)]


def edge_kernel(state_ref, phase_ref, last_ref, leading_ref, planes, phases, semaphores):
    length = state_ref.shape[1]
    sides = ((last_ref, length - WIDTH), (leading_ref, 0))
    copies = []
    for side, (_, start) in enumerate(sides):
        near = pl.ds(start, WIDTH)
        copies.append(pltpu.make_async_copy(state_ref.at[:, near], planes.at[side], semaphores.at[2 * side]))
        copies.append(pltpu.make_async_copy(phase_ref.at[near], phases.at[side], semaphores.at[2 * side + 1]))
    for copy in copies:
        copy.start()
    for side, (target, _) in enumerate(sides):
        copies[2 * side].wait()
        copies[2 * side + 1].wait()
        for k in range(WIDTH):
            state = [planes[side, member, k] for member in range(5)]
            velocity, press_now, *_ = point(state, phases[side, k])
            for member, piece in enumerate(flux(state, velocity, press_now, 0)):
                target[member, k] = piece


def rows_kernel(state_ref, phase_ref, rows_ref):
    rows = state_ref.shape[2]
    below = lax.broadcasted_iota(jnp.int32, (TILE, state_ref.shape[3]), 0) < TILE // 2

    def body(index, carry):
        state = []
        for member in range(5):
            first = state_ref[member, index, 0:TILE]
            final = state_ref[member, index, rows - TILE : rows]
            state.append(jnp.where(below, first, final))
        phase = jnp.where(below, phase_ref[index, 0:TILE], phase_ref[index, rows - TILE : rows])
        velocity, press_now, *_ = point(state, phase)
        for member, piece in enumerate(flux(state, velocity, press_now, 1)):
            rows_ref[member, index] = piece
        return carry

    lax.fori_loop(0, state_ref.shape[1], body, 0, unroll=2)


def middle_kernel(weights, first, final, coefs, state_ref, phase_ref, start_ref, before_ref, after_ref, out_ref, *rest):
    length, rows, lanes = phase_ref.shape
    xs, ys, zs = rest[-3:]
    blank = jnp.zeros((rows, lanes), jnp.float32)
    for member in range(5):
        for k in range(WIDTH):
            xs[member, k] = blank
            xs[member, WIDTH + length + k] = blank

    def fill(index, carry):
        state = plane(state_ref, index)
        velocity, press_now, *_ = point(state, phase_ref[index])
        for member, piece in enumerate(flux(state, velocity, press_now, 0)):
            xs[member, WIDTH + index] = piece
        for member, piece in enumerate(flux(state, velocity, press_now, 1)):
            ys[member, index, TILE : TILE + rows] = piece
            ys[member, index, 0:TILE] = before_ref[member, index]
            ys[member, index, TILE + rows : TILE + rows + TILE] = after_ref[member, index]
        for member, piece in enumerate(flux(state, velocity, press_now, 2)):
            zs[member, index] = piece
        return carry

    lax.fori_loop(0, length, fill, 0, unroll=2)
    keep, share = weights
    steps = [coefs[k] * share for k in range(3)]
    source = coefs[3] * share

    def update(index, carry):
        for member in range(5):
            third = zs[member, index]
            total = None
            for k in range(1, WIDTH + 1):
                ahead = xs[member, WIDTH + index + k] - xs[member, WIDTH + index - k]
                ahead = ahead + (
                    ys[member, index, TILE + k : TILE + k + rows] - ys[member, index, TILE - k : TILE - k + rows]
                )
                ahead = ahead + (pltpu.roll(third, lanes - k, 1) - pltpu.roll(third, k, 1))
                term = steps[k - 1] * ahead
                total = term if total is None else total + term
            value = state_ref[member, index]
            if first:
                value = value - total
            else:
                value = keep * start_ref[member, index] + (share * value - total)
            if member == 3:
                value = value + source * state_ref[0, index]
            if member == 4:
                value = value + source * state_ref[3, index]
            out_ref[member, index] = value
        return carry

    lax.fori_loop(0, length, update, 0)
    if final:

        def fastest(index, largest):
            return jnp.maximum(largest, wave_speed(plane(out_ref, index), phase_ref[index]))

        rest[0][...] = lax.fori_loop(WIDTH, length - WIDTH, fastest, blank)


def with_halo(share, coefs, partial_ref, left_ref, right_ref):
    length = partial_ref.shape[1]
    steps = [coefs[k] * share for k in range(3)]
    for near in range(WIDTH):
        left = plane(partial_ref, near)
        right = plane(partial_ref, length - 1 - near)
        for k in range(near + 1, WIDTH + 1):
            left = [v + steps[k - 1] * left_ref[m, WIDTH + near - k] for m, v in enumerate(left)]
            right = [v - steps[k - 1] * right_ref[m, k - 1 - near] for m, v in enumerate(right)]
        yield near, 0, near, left
        yield length - 1 - near, 1, WIDTH - 1 - near, right


def join_kernel(share, coefs, partial_ref, left_ref, right_ref, phase_ref, out_ref, last_ref, leading_ref):
    for index, side, place, state in with_halo(share, coefs, partial_ref, left_ref, right_ref):
        velocity, press_now, *_ = point(state, phase_ref[index])
        target = last_ref if side else leading_ref
        for member, piece in enumerate(flux(state, velocity, press_now, 0)):
            target[member, place] = piece
        for member in range(5):
            out_ref[member, index] = state[member]


def wave_speed(state, phase):
    velocity, press_now, inverse, gamma_cell, pinf_cell = point(state, phase)
    speed = jnp.abs(velocity[0]) + jnp.abs(velocity[1]) + jnp.abs(velocity[2])
    return speed + 3.0 * jnp.sqrt(gamma_cell * (press_now + pinf_cell) * inverse)


def final_kernel(
    share, coefs, partial_ref, left_ref, right_ref, phase_ref, inner_ref, out_ref, peak_ref, edges, semaphores
):
    length = partial_ref.shape[1]
    inner = pl.ds(WIDTH, length - 2 * WIDTH)
    copies = [pltpu.make_async_copy(partial_ref.at[:, inner], out_ref.at[:, inner], semaphores.at[0])]
    copies[0].start()
    largest = inner_ref[...]
    for index, side, place, state in with_halo(share, coefs, partial_ref, left_ref, right_ref):
        for member in range(5):
            edges[side, member, place] = state[member]
        largest = jnp.maximum(largest, wave_speed(state, phase_ref[index]))
    for side, start in enumerate((0, length - WIDTH)):
        copies.append(
            pltpu.make_async_copy(edges.at[side], out_ref.at[:, pl.ds(start, WIDTH)], semaphores.at[1 + side])
        )
        copies[-1].start()
    largest = jnp.max(largest, axis=0, keepdims=True)
    peak_ref[...] = jnp.broadcast_to(largest, peak_ref.shape)
    for copy in copies:
        copy.wait()


def peak_kernel(peaks_ref, largest_ref):
    largest = jnp.max(jnp.max(peaks_ref[...], axis=0, keepdims=True), axis=1, keepdims=True)
    largest_ref[...] = largest


def shaped(*shape):
    return jax.ShapeDtypeStruct(shape, jnp.float32)


def call(kernel, outs, specs, args, *, flops, scratch=(), aliases=None, places=None):
    moved = 4 * sum(math.prod(o.shape) for o in outs)
    return pl.pallas_call(
        kernel,
        out_shape=list(outs),
        in_specs=specs,
        out_specs=places or [VMEM] * len(outs),
        scratch_shapes=list(scratch),
        input_output_aliases=aliases or {},
        cost_estimate=pl.CostEstimate(flops=flops, bytes_accessed=moved, transcendentals=0),
        compiler_params=pltpu.CompilerParams(vmem_limit_bytes=16 << 20),
    )(*args)


def local(fields, phase_map, lagged_speed, step_count):
    _, length, rows, lanes = fields.shape
    cells = length * rows * lanes
    time_step = cfl_number / lagged_speed[0]
    gravity_now = gravity * (
        1.0 + shake_amp * jnp.cos(two_pi * step_count[0].astype(jnp.float32) / PERIOD)
    )
    coefs = time_step * jnp.stack(
        [jnp.float32(coef_one), jnp.float32(coef_two), jnp.float32(coef_three), gravity_now]
    )
    along, across = lax.axis_size("gx"), lax.axis_size("gy")
    up = [(i, (i + 1) % along) for i in range(along)]
    down = [(j, i) for i, j in up]
    over = [(i, (i + 1) % across) for i in range(across)]
    back = [(j, i) for i, j in over]
    edge = shaped(5, WIDTH, rows, lanes)
    whole = shaped(5, length, rows, lanes)
    row_tile = shaped(5, length, TILE, lanes)

    state = fields
    last, leading = call(
        edge_kernel,
        [edge, edge],
        [HBM, HBM],
        [pltpu.with_memory_space_constraint(array, pltpu.HBM) for array in (state, phase_map)],
        flops=cells * 20,
        scratch=[
            pltpu.VMEM((2, 5, WIDTH, rows, lanes), jnp.float32),
            pltpu.VMEM((2, WIDTH, rows, lanes), jnp.int32),
            pltpu.SemaphoreType.DMA((4,)),
        ],
    )
    stages = ((0.0, 1.0), (0.75, 0.25), (one_third, two_thirds))
    for number, weights in enumerate(stages):
        left = lax.ppermute(last, "gx", up)
        right = lax.ppermute(leading, "gx", down)
        (sent,) = call(rows_kernel, [row_tile], [VMEM, VMEM], [state, phase_map], flops=cells * 10)
        before = lax.ppermute(sent, "gy", over)
        after = before if across == 2 else lax.ppermute(sent, "gy", back)
        final = number == 2
        partial, *inner = call(
            functools.partial(middle_kernel, weights, number == 0, final),
            [whole, shaped(rows, lanes)] if final else [whole],
            [SMEM] + [VMEM] * 5,
            [coefs, state, phase_map, fields, before, after],
            flops=cells * 2000,
            scratch=[
                pltpu.VMEM((5, length + 2 * WIDTH, rows, lanes), jnp.float32),
                pltpu.VMEM((5, length, rows + 2 * TILE, lanes), jnp.float32),
                pltpu.VMEM((5, length, rows, lanes), jnp.float32),
            ],
        )
        if not final:
            state, last, leading = call(
                functools.partial(join_kernel, weights[1]),
                [whole, edge, edge],
                [SMEM] + [VMEM] * 4,
                [coefs, partial, left, right, phase_map],
                flops=cells * 20,
                aliases={1: 0},
            )
        else:
            advanced, peak = call(
                functools.partial(final_kernel, weights[1]),
                [whole, shaped(along * across, lanes)],
                [SMEM] + [VMEM] * 5,
                [coefs, partial, left, right, phase_map, *inner],
                flops=cells * 50,
                places=[HBM, VMEM],
                scratch=[
                    pltpu.VMEM((2, 5, WIDTH, rows, lanes), jnp.float32),
                    pltpu.SemaphoreType.DMA((3,)),
                ],
            )
    peaks = lax.all_to_all(peak, ("gx", "gy"), 0, 0, tiled=True)
    (largest,) = call(peak_kernel, [shaped(1, 1)], [VMEM], [peaks], flops=1000)
    return (advanced, jnp.reshape(largest, (1,)))


def solution(mesh):
    return jax.shard_map(
        local,
        mesh=mesh,
        in_specs=(P(None, "gx", "gy", None), P("gx", "gy", None), P(), P()),
        out_specs=(P(None, "gx", "gy", None), P()),
        check_vma=False,
    )
```

```python
import functools
import math

import jax
import jax.numpy as jnp
from jax import lax
from jax.experimental import pallas as pl
from jax.experimental.pallas import tpu as pltpu
from jax.sharding import PartitionSpec as P


PERIOD = 64


gamma_air = 1.4
gamma_water = 4.4
pinf_water = 3.0
cfl_number = 0.9
gravity = 1.0
shake_amp = 0.8
two_pi = 2.0 * math.pi
coef_one = 0.75
coef_two = -0.15
coef_three = 1.0 / 60.0
one_third = 1.0 / 3.0
two_thirds = 2.0 / 3.0

WIDTH = 3
TILE = 8
VMEM = pl.BlockSpec(memory_space=pltpu.VMEM)
HBM = pl.BlockSpec(memory_space=pltpu.HBM)


def point(state, phase):
    density, one, two, three, energy = state
    water_frac = phase.astype(jnp.float32)
    gamma_cell = gamma_air + (gamma_water - gamma_air) * water_frac
    pinf_cell = pinf_water * water_frac
    inverse = 1.0 / density
    velocity = (one * inverse, two * inverse, three * inverse)
    kinetic = 0.5 * (one * velocity[0] + two * velocity[1] + three * velocity[2])
    press_now = (gamma_cell - 1.0) * (energy - kinetic) - gamma_cell * pinf_cell
    return velocity, press_now, inverse, gamma_cell, pinf_cell


def flux(state, velocity, press_now, direction):
    speed = velocity[direction]
    pieces = [state[1 + direction]]
    for member in range(3):
        moment = state[1 + member] * speed
        pieces.append(moment + press_now if member == direction else moment)
    pieces.append((state[4] + press_now) * speed)
    return pieces


def plane(ref, index):
    return [ref[member, index] for member in range(5)]


def edge_kernel(state_ref, phase_ref, last_ref, leading_ref, planes, phases, semaphores):
    length = state_ref.shape[1]
    sides = ((last_ref, length - WIDTH), (leading_ref, 0))
    copies = []
    for side, (_, start) in enumerate(sides):
        near = pl.ds(start, WIDTH)
        copies.append(pltpu.make_async_copy(state_ref.at[:, near], planes.at[side], semaphores.at[2 * side]))
        copies.append(pltpu.make_async_copy(phase_ref.at[near], phases.at[side], semaphores.at[2 * side + 1]))
    for copy in copies:
        copy.start()
    for side, (target, _) in enumerate(sides):
        copies[2 * side].wait()
        copies[2 * side + 1].wait()
        for k in range(WIDTH):
            state = [planes[side, member, k] for member in range(5)]
            velocity, press_now, *_ = point(state, phases[side, k])
            for member, piece in enumerate(flux(state, velocity, press_now, 0)):
                target[member, k] = piece


def rows_kernel(state_ref, phase_ref, rows_ref):
    rows = state_ref.shape[2]
    below = lax.broadcasted_iota(jnp.int32, (TILE, state_ref.shape[3]), 0) < TILE // 2

    def body(index, carry):
        state = []
        for member in range(5):
            first = state_ref[member, index, 0:TILE]
            final = state_ref[member, index, rows - TILE : rows]
            state.append(jnp.where(below, first, final))
        phase = jnp.where(below, phase_ref[index, 0:TILE], phase_ref[index, rows - TILE : rows])
        velocity, press_now, *_ = point(state, phase)
        for member, piece in enumerate(flux(state, velocity, press_now, 1)):
            rows_ref[member, index] = piece
        return carry

    lax.fori_loop(0, state_ref.shape[1], body, 0, unroll=2)


def middle_kernel(weights, first, final, coefs, state_ref, phase_ref, start_ref, before_ref, after_ref, out_ref, *rest):
    length, rows, lanes = phase_ref.shape
    xs, ys, zs = rest[-3:]
    blank = jnp.zeros((rows, lanes), jnp.float32)
    for member in range(5):
        for k in range(WIDTH):
            xs[member, k] = blank
            xs[member, WIDTH + length + k] = blank

    def fill(index, carry):
        state = plane(state_ref, index)
        velocity, press_now, *_ = point(state, phase_ref[index])
        for member, piece in enumerate(flux(state, velocity, press_now, 0)):
            xs[member, WIDTH + index] = piece
        for member, piece in enumerate(flux(state, velocity, press_now, 1)):
            ys[member, index, TILE : TILE + rows] = piece
            ys[member, index, 0:TILE] = before_ref[member, index]
            ys[member, index, TILE + rows : TILE + rows + TILE] = after_ref[member, index]
        for member, piece in enumerate(flux(state, velocity, press_now, 2)):
            zs[member, index] = piece
        return carry

    lax.fori_loop(0, length, fill, 0, unroll=2)
    keep, share = weights
    steps = [coefs[k] * share for k in range(3)]
    source = coefs[3] * share

    def update(index, carry):
        for member in range(5):
            third = zs[member, index]
            total = None
            for k in range(1, WIDTH + 1):
                ahead = xs[member, WIDTH + index + k] - xs[member, WIDTH + index - k]
                ahead = ahead + (
                    ys[member, index, TILE + k : TILE + k + rows] - ys[member, index, TILE - k : TILE - k + rows]
                )
                ahead = ahead + (pltpu.roll(third, lanes - k, 1) - pltpu.roll(third, k, 1))
                term = steps[k - 1] * ahead
                total = term if total is None else total + term
            value = state_ref[member, index]
            if first:
                value = value - total
            else:
                value = keep * start_ref[member, index] + (share * value - total)
            if member == 3:
                value = value + source * state_ref[0, index]
            if member == 4:
                value = value + source * state_ref[3, index]
            out_ref[member, index] = value
        return carry

    lax.fori_loop(0, length, update, 0)
    if final:

        def fastest(index, largest):
            return jnp.maximum(largest, wave_speed(plane(out_ref, index), phase_ref[index]))

        rest[0][...] = lax.fori_loop(WIDTH, length - WIDTH, fastest, blank)


def with_halo(share, coefs, partial_ref, left_ref, right_ref):
    length = partial_ref.shape[1]
    steps = [coefs[k] * share for k in range(3)]
    for near in range(WIDTH):
        left = plane(partial_ref, near)
        right = plane(partial_ref, length - 1 - near)
        for k in range(near + 1, WIDTH + 1):
            left = [v + steps[k - 1] * left_ref[m, WIDTH + near - k] for m, v in enumerate(left)]
            right = [v - steps[k - 1] * right_ref[m, k - 1 - near] for m, v in enumerate(right)]
        yield near, 0, near, left
        yield length - 1 - near, 1, WIDTH - 1 - near, right


def join_kernel(share, coefs, partial_ref, left_ref, right_ref, phase_ref, out_ref, last_ref, leading_ref):
    for index, side, place, state in with_halo(share, coefs, partial_ref, left_ref, right_ref):
        velocity, press_now, *_ = point(state, phase_ref[index])
        target = last_ref if side else leading_ref
        for member, piece in enumerate(flux(state, velocity, press_now, 0)):
            target[member, place] = piece
        for member in range(5):
            out_ref[member, index] = state[member]


def wave_speed(state, phase):
    velocity, press_now, inverse, gamma_cell, pinf_cell = point(state, phase)
    speed = jnp.abs(velocity[0]) + jnp.abs(velocity[1]) + jnp.abs(velocity[2])
    return speed + 3.0 * jnp.sqrt(gamma_cell * (press_now + pinf_cell) * inverse)


def final_kernel(
    share, coefs, partial_ref, left_ref, right_ref, phase_ref, inner_ref, out_ref, peak_ref, edges, semaphores
):
    length = partial_ref.shape[1]
    inner = pl.ds(WIDTH, length - 2 * WIDTH)
    copies = [pltpu.make_async_copy(partial_ref.at[:, inner], out_ref.at[:, inner], semaphores.at[0])]
    copies[0].start()
    largest = inner_ref[...]
    for index, side, place, state in with_halo(share, coefs, partial_ref, left_ref, right_ref):
        for member in range(5):
            edges[side, member, place] = state[member]
        largest = jnp.maximum(largest, wave_speed(state, phase_ref[index]))
    for side, start in enumerate((0, length - WIDTH)):
        copies.append(
            pltpu.make_async_copy(edges.at[side], out_ref.at[:, pl.ds(start, WIDTH)], semaphores.at[1 + side])
        )
        copies[-1].start()
    largest = jnp.max(largest, axis=0, keepdims=True)
    peak_ref[...] = jnp.broadcast_to(largest, peak_ref.shape)
    for copy in copies:
        copy.wait()


def peak_kernel(peaks_ref, largest_ref):
    largest = jnp.max(jnp.max(peaks_ref[...], axis=0, keepdims=True), axis=1, keepdims=True)
    largest_ref[...] = largest


def shaped(*shape):
    return jax.ShapeDtypeStruct(shape, jnp.float32)


def call(kernel, outs, specs, args, *, flops, scratch=(), aliases=None, places=None):
    moved = 4 * sum(math.prod(o.shape) for o in outs)
    return pl.pallas_call(
        kernel,
        out_shape=list(outs),
        in_specs=specs,
        out_specs=places or [VMEM] * len(outs),
        scratch_shapes=list(scratch),
        input_output_aliases=aliases or {},
        cost_estimate=pl.CostEstimate(flops=flops, bytes_accessed=moved, transcendentals=0),
        compiler_params=pltpu.CompilerParams(vmem_limit_bytes=16 << 20),
    )(*args)


def local(fields, phase_map, lagged_speed, step_count):
    _, length, rows, lanes = fields.shape
    cells = length * rows * lanes
    time_step = cfl_number / lagged_speed[0]
    gravity_now = gravity * (
        1.0 + shake_amp * jnp.cos(two_pi * step_count[0].astype(jnp.float32) / PERIOD)
    )
    coefs = time_step * jnp.stack(
        [jnp.float32(coef_one), jnp.float32(coef_two), jnp.float32(coef_three), gravity_now]
    )
    coefs = jnp.broadcast_to(coefs[:, None, None], (4, rows, lanes))
    along, across = lax.axis_size("gx"), lax.axis_size("gy")
    up = [(i, (i + 1) % along) for i in range(along)]
    down = [(j, i) for i, j in up]
    over = [(i, (i + 1) % across) for i in range(across)]
    back = [(j, i) for i, j in over]
    edge = shaped(5, WIDTH, rows, lanes)
    whole = shaped(5, length, rows, lanes)
    row_tile = shaped(5, length, TILE, lanes)

    state = fields
    last, leading = call(
        edge_kernel,
        [edge, edge],
        [HBM, HBM],
        [pltpu.with_memory_space_constraint(array, pltpu.HBM) for array in (state, phase_map)],
        flops=cells * 20,
        scratch=[
            pltpu.VMEM((2, 5, WIDTH, rows, lanes), jnp.float32),
            pltpu.VMEM((2, WIDTH, rows, lanes), jnp.int32),
            pltpu.SemaphoreType.DMA((4,)),
        ],
    )
    stages = ((0.0, 1.0), (0.75, 0.25), (one_third, two_thirds))
    for number, weights in enumerate(stages):
        left = lax.ppermute(last, "gx", up)
        right = lax.ppermute(leading, "gx", down)
        (sent,) = call(rows_kernel, [row_tile], [VMEM, VMEM], [state, phase_map], flops=cells * 10)
        before = lax.ppermute(sent, "gy", over)
        after = before if across == 2 else lax.ppermute(sent, "gy", back)
        final = number == 2
        partial, *inner = call(
            functools.partial(middle_kernel, weights, number == 0, final),
            [whole, shaped(rows, lanes)] if final else [whole],
            [VMEM] * 6,
            [coefs, state, phase_map, fields, before, after],
            flops=cells * 2000,
            scratch=[
                pltpu.VMEM((5, length + 2 * WIDTH, rows, lanes), jnp.float32),
                pltpu.VMEM((5, length, rows + 2 * TILE, lanes), jnp.float32),
                pltpu.VMEM((5, length, rows, lanes), jnp.float32),
            ],
        )
        if not final:
            state, last, leading = call(
                functools.partial(join_kernel, weights[1]),
                [whole, edge, edge],
                [VMEM] * 5,
                [coefs, partial, left, right, phase_map],
                flops=cells * 20,
                aliases={1: 0},
            )
        else:
            advanced, peak = call(
                functools.partial(final_kernel, weights[1]),
                [whole, shaped(along * across, lanes)],
                [VMEM] * 6,
                [coefs, partial, left, right, phase_map, *inner],
                flops=cells * 50,
                places=[HBM, VMEM],
                scratch=[
                    pltpu.VMEM((2, 5, WIDTH, rows, lanes), jnp.float32),
                    pltpu.SemaphoreType.DMA((3,)),
                ],
            )
    peaks = lax.all_to_all(peak, ("gx", "gy"), 0, 0, tiled=True)
    (largest,) = call(peak_kernel, [shaped(1, 1)], [VMEM], [peaks], flops=1000)
    return (advanced, jnp.reshape(largest, (1,)))


def solution(mesh):
    return jax.shard_map(
        local,
        mesh=mesh,
        in_specs=(P(None, "gx", "gy", None), P("gx", "gy", None), P(), P()),
        out_specs=(P(None, "gx", "gy", None), P()),
        check_vma=False,
    )
```

```python
import functools
import math

import jax
import jax.numpy as jnp
from jax import lax
from jax.experimental import pallas as pl
from jax.experimental.pallas import tpu as pltpu
from jax.sharding import PartitionSpec as P


PERIOD = 64


gamma_air = 1.4
gamma_water = 4.4
pinf_water = 3.0
cfl_number = 0.9
gravity = 1.0
shake_amp = 0.8
two_pi = 2.0 * math.pi
coef_one = 0.75
coef_two = -0.15
coef_three = 1.0 / 60.0
one_third = 1.0 / 3.0
two_thirds = 2.0 / 3.0

STAGES = (
    (("up", "down"), (0.0, 1.0)),
    (("down", "up"), (0.75, 0.25)),
    (("up", "down"), (one_third, two_thirds)),
)
WIDTH = 3
TILE = 8
VMEM = pl.BlockSpec(memory_space=pltpu.VMEM)
HBM = pl.BlockSpec(memory_space=pltpu.HBM)


def point(state, phase):
    density, one, two, three, energy = state
    water_frac = phase.astype(jnp.float32)
    gamma_cell = gamma_air + (gamma_water - gamma_air) * water_frac
    pinf_cell = pinf_water * water_frac
    inverse = 1.0 / density
    velocity = (one * inverse, two * inverse, three * inverse)
    kinetic = 0.5 * (one * velocity[0] + two * velocity[1] + three * velocity[2])
    press_now = (gamma_cell - 1.0) * (energy - kinetic) - gamma_cell * pinf_cell
    return velocity, press_now, inverse, gamma_cell, pinf_cell


def flux(state, velocity, press_now, direction):
    speed = velocity[direction]
    pieces = [state[1 + direction]]
    for member in range(3):
        moment = state[1 + member] * speed
        pieces.append(moment + press_now if member == direction else moment)
    pieces.append((state[4] + press_now) * speed)
    return pieces


def plane(ref, index):
    return [ref[member, index] for member in range(5)]


def edge_kernel(state_ref, phase_ref, last_ref, leading_ref, planes, phases, semaphores):
    length = state_ref.shape[1]
    sides = ((last_ref, length - WIDTH), (leading_ref, 0))
    copies = []
    for side, (_, start) in enumerate(sides):
        near = pl.ds(start, WIDTH)
        copies.append(pltpu.make_async_copy(state_ref.at[:, near], planes.at[side], semaphores.at[2 * side]))
        copies.append(pltpu.make_async_copy(phase_ref.at[near], phases.at[side], semaphores.at[2 * side + 1]))
    for copy in copies:
        copy.start()
    for side, (target, _) in enumerate(sides):
        copies[2 * side].wait()
        copies[2 * side + 1].wait()
        for k in range(WIDTH):
            state = [planes[side, member, k] for member in range(5)]
            velocity, press_now, *_ = point(state, phases[side, k])
            for member, piece in enumerate(flux(state, velocity, press_now, 0)):
                target[member, k] = piece


def rows_kernel(state_ref, phase_ref, rows_ref):
    rows = state_ref.shape[2]
    below = lax.broadcasted_iota(jnp.int32, (TILE, state_ref.shape[3]), 0) < TILE // 2

    def body(index, carry):
        state = []
        for member in range(5):
            first = state_ref[member, index, 0:TILE]
            final = state_ref[member, index, rows - TILE : rows]
            state.append(jnp.where(below, first, final))
        phase = jnp.where(below, phase_ref[index, 0:TILE], phase_ref[index, rows - TILE : rows])
        velocity, press_now, *_ = point(state, phase)
        for member, piece in enumerate(flux(state, velocity, press_now, 1)):
            rows_ref[member, index] = piece
        return carry

    lax.fori_loop(0, state_ref.shape[1], body, 0, unroll=2)


def middle_kernel(weights, first, final, coefs, state_ref, phase_ref, start_ref, before_ref, after_ref, out_ref, *rest):
    length, rows, lanes = phase_ref.shape
    xs, ys, zs = rest[-3:]
    blank = jnp.zeros((rows, lanes), jnp.float32)
    for member in range(5):
        for k in range(WIDTH):
            xs[member, k] = blank
            xs[member, WIDTH + length + k] = blank

    def fill(index, carry):
        state = plane(state_ref, index)
        velocity, press_now, *_ = point(state, phase_ref[index])
        for member, piece in enumerate(flux(state, velocity, press_now, 0)):
            xs[member, WIDTH + index] = piece
        for member, piece in enumerate(flux(state, velocity, press_now, 1)):
            ys[member, index, TILE : TILE + rows] = piece
            ys[member, index, 0:TILE] = before_ref[member, index]
            ys[member, index, TILE + rows : TILE + rows + TILE] = after_ref[member, index]
        for member, piece in enumerate(flux(state, velocity, press_now, 2)):
            zs[member, index] = piece
        return carry

    lax.fori_loop(0, length, fill, 0, unroll=2)
    keep, share = weights
    steps = [coefs[k] * share for k in range(3)]
    source = coefs[3] * share

    def update(index, carry):
        for member in range(5):
            third = zs[member, index]
            total = None
            for k in range(1, WIDTH + 1):
                ahead = xs[member, WIDTH + index + k] - xs[member, WIDTH + index - k]
                ahead = ahead + (
                    ys[member, index, TILE + k : TILE + k + rows] - ys[member, index, TILE - k : TILE - k + rows]
                )
                ahead = ahead + (pltpu.roll(third, lanes - k, 1) - pltpu.roll(third, k, 1))
                term = steps[k - 1] * ahead
                total = term if total is None else total + term
            value = state_ref[member, index]
            if first:
                value = value - total
            else:
                value = keep * start_ref[member, index] + (share * value - total)
            if member == 3:
                value = value + source * state_ref[0, index]
            if member == 4:
                value = value + source * state_ref[3, index]
            out_ref[member, index] = value
        return carry

    lax.fori_loop(0, length, update, 0)
    if final:

        def fastest(index, largest):
            return jnp.maximum(largest, wave_speed(plane(out_ref, index), phase_ref[index]))

        rest[0][...] = lax.fori_loop(WIDTH, length - WIDTH, fastest, blank)


def with_halo(share, coefs, partial_ref, halo_ref, above):
    length = partial_ref.shape[1]
    steps = [coefs[k] * (-share if above else share) for k in range(3)]
    for near in range(WIDTH):
        index = length - 1 - near if above else near
        state = plane(partial_ref, index)
        for k in range(near + 1, WIDTH + 1):
            place = k - 1 - near if above else WIDTH + near - k
            state = [value + steps[k - 1] * halo_ref[member, place] for member, value in enumerate(state)]
        yield index, WIDTH - 1 - near if above else near, state


def join_kernel(share, above, coefs, partial_ref, halo_ref, phase_ref, out_ref, edge_ref):
    for index, place, state in with_halo(share, coefs, partial_ref, halo_ref, above):
        velocity, press_now, *_ = point(state, phase_ref[index])
        for member, piece in enumerate(flux(state, velocity, press_now, 0)):
            edge_ref[member, place] = piece
        for member in range(5):
            out_ref[member, index] = state[member]


def wave_speed(state, phase):
    velocity, press_now, inverse, gamma_cell, pinf_cell = point(state, phase)
    speed = jnp.abs(velocity[0]) + jnp.abs(velocity[1]) + jnp.abs(velocity[2])
    return speed + 3.0 * jnp.sqrt(gamma_cell * (press_now + pinf_cell) * inverse)


def final_kernel(
    share, coefs, partial_ref, left_ref, right_ref, phase_ref, inner_ref, out_ref, peak_ref, edges, semaphores
):
    length = partial_ref.shape[1]
    inner = pl.ds(WIDTH, length - 2 * WIDTH)
    copies = [pltpu.make_async_copy(partial_ref.at[:, inner], out_ref.at[:, inner], semaphores.at[0])]
    copies[0].start()
    largest = inner_ref[...]
    for side, halo_ref in enumerate((left_ref, right_ref)):
        for index, place, state in with_halo(share, coefs, partial_ref, halo_ref, side == 1):
            for member in range(5):
                edges[side, member, place] = state[member]
            largest = jnp.maximum(largest, wave_speed(state, phase_ref[index]))
    for side, start in enumerate((0, length - WIDTH)):
        copies.append(
            pltpu.make_async_copy(edges.at[side], out_ref.at[:, pl.ds(start, WIDTH)], semaphores.at[1 + side])
        )
        copies[-1].start()
    largest = jnp.max(largest, axis=0, keepdims=True)
    peak_ref[...] = jnp.broadcast_to(largest, peak_ref.shape)
    for copy in copies:
        copy.wait()


def peak_kernel(peaks_ref, largest_ref):
    largest = jnp.max(jnp.max(peaks_ref[...], axis=0, keepdims=True), axis=1, keepdims=True)
    largest_ref[...] = largest


def shaped(*shape):
    return jax.ShapeDtypeStruct(shape, jnp.float32)


def call(kernel, outs, specs, args, *, flops, scratch=(), aliases=None, places=None):
    moved = 4 * sum(math.prod(o.shape) for o in outs)
    return pl.pallas_call(
        kernel,
        out_shape=list(outs),
        in_specs=specs,
        out_specs=places or [VMEM] * len(outs),
        scratch_shapes=list(scratch),
        input_output_aliases=aliases or {},
        cost_estimate=pl.CostEstimate(flops=flops, bytes_accessed=moved, transcendentals=0),
        compiler_params=pltpu.CompilerParams(vmem_limit_bytes=16 << 20),
    )(*args)


def advance(fields, phase_map, lagged_speed, step_count):
    _, length, rows, lanes = fields.shape
    cells = length * rows * lanes
    time_step = cfl_number / lagged_speed[0]
    gravity_now = gravity * (
        1.0 + shake_amp * jnp.cos(two_pi * step_count[0].astype(jnp.float32) / PERIOD)
    )
    coefs = time_step * jnp.stack(
        [jnp.float32(coef_one), jnp.float32(coef_two), jnp.float32(coef_three), gravity_now]
    )
    coefs = jnp.broadcast_to(coefs[:, None, None], (4, rows, lanes))
    along, across = lax.axis_size("gx"), lax.axis_size("gy")
    up = [(i, (i + 1) % along) for i in range(along)]
    down = [(j, i) for i, j in up]
    over = [(i, (i + 1) % across) for i in range(across)]
    back = [(j, i) for i, j in over]
    edge = shaped(5, WIDTH, rows, lanes)
    whole = shaped(5, length, rows, lanes)
    row_tile = shaped(5, length, TILE, lanes)

    state = fields
    last, leading = call(
        edge_kernel,
        [edge, edge],
        [HBM, HBM],
        [pltpu.with_memory_space_constraint(array, pltpu.HBM) for array in (state, phase_map)],
        flops=cells * 20,
        scratch=[
            pltpu.VMEM((2, 5, WIDTH, rows, lanes), jnp.float32),
            pltpu.VMEM((2, WIDTH, rows, lanes), jnp.int32),
            pltpu.SemaphoreType.DMA((4,)),
        ],
    )
    edges = {"up": last, "down": leading}
    for number, ((first, second), weights) in enumerate(STAGES):
        halos = {}
        for way in (first, second):
            halos[way] = lax.ppermute(edges[way], "gx", up if way == "up" else down)
        (sent,) = call(rows_kernel, [row_tile], [VMEM, VMEM], [state, phase_map], flops=cells * 10)
        before = lax.ppermute(sent, "gy", over)
        after = before if across == 2 else lax.ppermute(sent, "gy", back)
        final = number == len(STAGES) - 1
        state, *inner = call(
            functools.partial(middle_kernel, weights, number == 0, final),
            [whole, shaped(rows, lanes)] if final else [whole],
            [VMEM] * 6,
            [coefs, state, phase_map, fields, before, after],
            flops=cells * 2000,
            scratch=[
                pltpu.VMEM((5, length + 2 * WIDTH, rows, lanes), jnp.float32),
                pltpu.VMEM((5, length, rows + 2 * TILE, lanes), jnp.float32),
                pltpu.VMEM((5, length, rows, lanes), jnp.float32),
            ],
        )
        if final:
            advanced, peak = call(
                functools.partial(final_kernel, weights[1]),
                [whole, shaped(along * across, lanes)],
                [VMEM] * 6,
                [coefs, state, halos["up"], halos["down"], phase_map, *inner],
                flops=cells * 50,
                places=[HBM, VMEM],
                scratch=[
                    pltpu.VMEM((2, 5, WIDTH, rows, lanes), jnp.float32),
                    pltpu.SemaphoreType.DMA((3,)),
                ],
            )
            break
        for way in STAGES[number + 1][0]:
            above = way == "up"
            state, edges[way] = call(
                functools.partial(join_kernel, weights[1], above),
                [whole, edge],
                [VMEM] * 4,
                [coefs, state, halos["down" if above else "up"], phase_map],
                flops=cells * 10,
                aliases={1: 0},
            )
    peaks = lax.all_to_all(peak, ("gx", "gy"), 0, 0, tiled=True)
    (largest,) = call(peak_kernel, [shaped(1, 1)], [VMEM], [peaks], flops=1000)
    return (advanced, jnp.reshape(largest, (1,)))


def solution(mesh):
    return jax.shard_map(
        advance,
        mesh=mesh,
        in_specs=(P(None, "gx", "gy", None), P("gx", "gy", None), P(), P()),
        out_specs=(P(None, "gx", "gy", None), P()),
        check_vma=False,
    )
```

```python
import functools
import math

import jax
import jax.numpy as jnp
from jax import lax
from jax.experimental import pallas as pl
from jax.experimental.pallas import tpu as pltpu
from jax.sharding import PartitionSpec as P


PERIOD = 64


gamma_air = 1.4
gamma_water = 4.4
pinf_water = 3.0
cfl_number = 0.9
gravity = 1.0
shake_amp = 0.8
two_pi = 2.0 * math.pi
coef_one = 0.75
coef_two = -0.15
coef_three = 1.0 / 60.0
one_third = 1.0 / 3.0
two_thirds = 2.0 / 3.0

STAGES = (
    (("up", "down"), (0.0, 1.0)),
    (("down", "up"), (0.75, 0.25)),
    (("up", "down"), (one_third, two_thirds)),
)
WIDTH = 3
TILE = 8
VMEM = pl.BlockSpec(memory_space=pltpu.VMEM)
HBM = pl.BlockSpec(memory_space=pltpu.HBM)


def point(state, phase):
    density, one, two, three, energy = state
    water_frac = phase.astype(jnp.float32)
    gamma_cell = gamma_air + (gamma_water - gamma_air) * water_frac
    pinf_cell = pinf_water * water_frac
    inverse = 1.0 / density
    velocity = (one * inverse, two * inverse, three * inverse)
    kinetic = 0.5 * (one * velocity[0] + two * velocity[1] + three * velocity[2])
    press_now = (gamma_cell - 1.0) * (energy - kinetic) - gamma_cell * pinf_cell
    return velocity, press_now, inverse, gamma_cell, pinf_cell


def flux(state, velocity, press_now, direction):
    speed = velocity[direction]
    pieces = [state[1 + direction]]
    for member in range(3):
        moment = state[1 + member] * speed
        pieces.append(moment + press_now if member == direction else moment)
    pieces.append((state[4] + press_now) * speed)
    return pieces


def plane(ref, index):
    return [ref[member, index] for member in range(5)]


def edge_kernel(state_ref, phase_ref, last_ref, leading_ref, planes, phases, semaphores):
    length = state_ref.shape[1]
    sides = ((last_ref, length - WIDTH), (leading_ref, 0))
    copies = []
    for side, (_, start) in enumerate(sides):
        near = pl.ds(start, WIDTH)
        copies.append(pltpu.make_async_copy(state_ref.at[:, near], planes.at[side], semaphores.at[2 * side]))
        copies.append(pltpu.make_async_copy(phase_ref.at[near], phases.at[side], semaphores.at[2 * side + 1]))
    for copy in copies:
        copy.start()
    for side, (target, _) in enumerate(sides):
        copies[2 * side].wait()
        copies[2 * side + 1].wait()
        for k in range(WIDTH):
            state = [planes[side, member, k] for member in range(5)]
            velocity, press_now, *_ = point(state, phases[side, k])
            for member, piece in enumerate(flux(state, velocity, press_now, 0)):
                target[member, k] = piece


def rows_kernel(state_ref, phase_ref, rows_ref):
    rows = state_ref.shape[2]
    below = lax.broadcasted_iota(jnp.int32, (TILE, state_ref.shape[3]), 0) < TILE // 2

    def body(index, carry):
        state = []
        for member in range(5):
            first = state_ref[member, index, 0:TILE]
            final = state_ref[member, index, rows - TILE : rows]
            state.append(jnp.where(below, first, final))
        phase = jnp.where(below, phase_ref[index, 0:TILE], phase_ref[index, rows - TILE : rows])
        velocity, press_now, *_ = point(state, phase)
        for member, piece in enumerate(flux(state, velocity, press_now, 1)):
            rows_ref[member, index] = piece
        return carry

    lax.fori_loop(0, state_ref.shape[1], body, 0, unroll=2)


def middle_kernel(weights, first, coefs, state_ref, phase_ref, start_ref, out_ref, xs, ys, zs):
    length, rows, lanes = phase_ref.shape
    blank = jnp.zeros((rows, lanes), jnp.float32)
    for member in range(5):
        for k in range(WIDTH):
            xs[member, k] = blank
            xs[member, WIDTH + length + k] = blank

    def fill(index, carry):
        state = plane(state_ref, index)
        velocity, press_now, *_ = point(state, phase_ref[index])
        for member, piece in enumerate(flux(state, velocity, press_now, 0)):
            xs[member, WIDTH + index] = piece
        for member, piece in enumerate(flux(state, velocity, press_now, 1)):
            ys[member, index, TILE : TILE + rows] = piece
            ys[member, index, 0:TILE] = blank[0:TILE]
            ys[member, index, TILE + rows : TILE + rows + TILE] = blank[0:TILE]
        for member, piece in enumerate(flux(state, velocity, press_now, 2)):
            zs[member, index] = piece
        return carry

    lax.fori_loop(0, length, fill, 0, unroll=2)
    keep, share = weights
    steps = [coefs[k] * share for k in range(3)]
    source = coefs[3] * share

    def update(index, carry):
        for member in range(5):
            third = zs[member, index]
            total = None
            for k in range(1, WIDTH + 1):
                ahead = xs[member, WIDTH + index + k] - xs[member, WIDTH + index - k]
                ahead = ahead + (
                    ys[member, index, TILE + k : TILE + k + rows] - ys[member, index, TILE - k : TILE - k + rows]
                )
                ahead = ahead + (pltpu.roll(third, lanes - k, 1) - pltpu.roll(third, k, 1))
                term = steps[k - 1] * ahead
                total = term if total is None else total + term
            value = state_ref[member, index]
            if first:
                value = value - total
            else:
                value = keep * start_ref[member, index] + (share * value - total)
            if member == 3:
                value = value + source * state_ref[0, index]
            if member == 4:
                value = value + source * state_ref[3, index]
            out_ref[member, index] = value
        return carry

    lax.fori_loop(0, length, update, 0, unroll=4)


def border_kernel(share, final, coefs, partial_ref, phase_ref, before_ref, after_ref, out_ref, *inner_ref):
    _, length, rows, lanes = partial_ref.shape
    place = lax.broadcasted_iota(jnp.int32, (TILE, lanes), 0)
    blank = jnp.zeros((TILE, lanes), jnp.float32)
    steps = [coefs[k, 0:TILE] * share for k in range(3)]
    early = [jnp.where(place < k, steps[k - 1], blank) for k in range(1, WIDTH + 1)]
    late = [jnp.where(place >= TILE - k, steps[k - 1], blank) for k in range(1, WIDTH + 1)]

    def border(index, carry):
        for member in range(5):
            before, after = before_ref[member, index], after_ref[member, index]
            first = partial_ref[member, index, 0:TILE]
            final = partial_ref[member, index, rows - TILE : rows]
            for k in range(1, WIDTH + 1):
                first = first + early[k - 1] * pltpu.roll(before, k, 0)
                final = final - late[k - 1] * pltpu.roll(after, TILE - k, 0)
            out_ref[member, index, 0:TILE] = first
            out_ref[member, index, rows - TILE : rows] = final
        return carry

    lax.fori_loop(0, length, border, 0, unroll=2)
    if final:

        def fastest(index, largest):
            return jnp.maximum(largest, wave_speed(plane(out_ref, index), phase_ref[index]))

        blank = jnp.zeros((rows, lanes), jnp.float32)
        inner_ref[0][...] = lax.fori_loop(WIDTH, length - WIDTH, fastest, blank, unroll=2)


def with_halo(share, coefs, partial_ref, halo_ref, above):
    length = partial_ref.shape[1]
    steps = [coefs[k] * (-share if above else share) for k in range(3)]
    for near in range(WIDTH):
        index = length - 1 - near if above else near
        state = plane(partial_ref, index)
        for k in range(near + 1, WIDTH + 1):
            place = k - 1 - near if above else WIDTH + near - k
            state = [value + steps[k - 1] * halo_ref[member, place] for member, value in enumerate(state)]
        yield index, WIDTH - 1 - near if above else near, state


def join_kernel(share, above, coefs, partial_ref, halo_ref, phase_ref, out_ref, edge_ref):
    for index, place, state in with_halo(share, coefs, partial_ref, halo_ref, above):
        velocity, press_now, *_ = point(state, phase_ref[index])
        for member, piece in enumerate(flux(state, velocity, press_now, 0)):
            edge_ref[member, place] = piece
        for member in range(5):
            out_ref[member, index] = state[member]


def wave_speed(state, phase):
    velocity, press_now, inverse, gamma_cell, pinf_cell = point(state, phase)
    speed = jnp.abs(velocity[0]) + jnp.abs(velocity[1]) + jnp.abs(velocity[2])
    return speed + 3.0 * jnp.sqrt(gamma_cell * (press_now + pinf_cell) * inverse)


def final_kernel(
    share, coefs, partial_ref, left_ref, right_ref, phase_ref, inner_ref, out_ref, peak_ref, edges, semaphores
):
    length = partial_ref.shape[1]
    inner = pl.ds(WIDTH, length - 2 * WIDTH)
    copies = [pltpu.make_async_copy(partial_ref.at[:, inner], out_ref.at[:, inner], semaphores.at[0])]
    copies[0].start()
    largest = inner_ref[...]
    for side, halo_ref in enumerate((left_ref, right_ref)):
        for index, place, state in with_halo(share, coefs, partial_ref, halo_ref, side == 1):
            for member in range(5):
                edges[side, member, place] = state[member]
            largest = jnp.maximum(largest, wave_speed(state, phase_ref[index]))
    for side, start in enumerate((0, length - WIDTH)):
        copies.append(
            pltpu.make_async_copy(edges.at[side], out_ref.at[:, pl.ds(start, WIDTH)], semaphores.at[1 + side])
        )
        copies[-1].start()
    largest = jnp.max(largest, axis=0, keepdims=True)
    peak_ref[...] = jnp.broadcast_to(largest, peak_ref.shape)
    for copy in copies:
        copy.wait()


def peak_kernel(peaks_ref, largest_ref):
    largest = jnp.max(jnp.max(peaks_ref[...], axis=0, keepdims=True), axis=1, keepdims=True)
    largest_ref[...] = largest


def shaped(*shape):
    return jax.ShapeDtypeStruct(shape, jnp.float32)


def call(kernel, outs, specs, args, *, flops, scratch=(), aliases=None, places=None):
    moved = 4 * sum(math.prod(o.shape) for o in outs)
    return pl.pallas_call(
        kernel,
        out_shape=list(outs),
        in_specs=specs,
        out_specs=places or [VMEM] * len(outs),
        scratch_shapes=list(scratch),
        input_output_aliases=aliases or {},
        cost_estimate=pl.CostEstimate(flops=flops, bytes_accessed=moved, transcendentals=0),
        compiler_params=pltpu.CompilerParams(vmem_limit_bytes=16 << 20),
    )(*args)


def advance(fields, phase_map, lagged_speed, step_count):
    _, length, rows, lanes = fields.shape
    cells = length * rows * lanes
    time_step = cfl_number / lagged_speed[0]
    gravity_now = gravity * (
        1.0 + shake_amp * jnp.cos(two_pi * step_count[0].astype(jnp.float32) / PERIOD)
    )
    coefs = time_step * jnp.stack(
        [jnp.float32(coef_one), jnp.float32(coef_two), jnp.float32(coef_three), gravity_now]
    )
    coefs = jnp.broadcast_to(coefs[:, None, None], (4, rows, lanes))
    along, across = lax.axis_size("gx"), lax.axis_size("gy")
    up = [(i, (i + 1) % along) for i in range(along)]
    down = [(j, i) for i, j in up]
    over = [(i, (i + 1) % across) for i in range(across)]
    back = [(j, i) for i, j in over]
    edge = shaped(5, WIDTH, rows, lanes)
    whole = shaped(5, length, rows, lanes)
    row_tile = shaped(5, length, TILE, lanes)

    state = fields
    last, leading = call(
        edge_kernel,
        [edge, edge],
        [HBM, HBM],
        [pltpu.with_memory_space_constraint(array, pltpu.HBM) for array in (state, phase_map)],
        flops=cells * 20,
        scratch=[
            pltpu.VMEM((2, 5, WIDTH, rows, lanes), jnp.float32),
            pltpu.VMEM((2, WIDTH, rows, lanes), jnp.int32),
            pltpu.SemaphoreType.DMA((4,)),
        ],
    )
    edges = {"up": last, "down": leading}
    for number, ((first, second), weights) in enumerate(STAGES):
        halos = {}
        for way in (first, second):
            halos[way] = lax.ppermute(edges[way], "gx", up if way == "up" else down)
        (sent,) = call(rows_kernel, [row_tile], [VMEM, VMEM], [state, phase_map], flops=cells * 10)
        before = lax.ppermute(sent, "gy", over)
        after = before if across == 2 else lax.ppermute(sent, "gy", back)
        final = number == len(STAGES) - 1
        (state,) = call(
            functools.partial(middle_kernel, weights, number == 0),
            [whole],
            [VMEM] * 4,
            [coefs, state, phase_map, fields],
            flops=cells * 1000,
            scratch=[
                pltpu.VMEM((5, length + 2 * WIDTH, rows, lanes), jnp.float32),
                pltpu.VMEM((5, length, rows + 2 * TILE, lanes), jnp.float32),
                pltpu.VMEM((5, length, rows, lanes), jnp.float32),
            ],
        )
        state, *inner = call(
            functools.partial(border_kernel, weights[1], final),
            [whole, shaped(rows, lanes)] if final else [whole],
            [VMEM] * 5,
            [coefs, state, phase_map, before, after],
            flops=cells * 20,
            aliases={1: 0},
        )
        if final:
            advanced, peak = call(
                functools.partial(final_kernel, weights[1]),
                [whole, shaped(along * across, lanes)],
                [VMEM] * 6,
                [coefs, state, halos["up"], halos["down"], phase_map, *inner],
                flops=cells * 50,
                places=[HBM, VMEM],
                scratch=[
                    pltpu.VMEM((2, 5, WIDTH, rows, lanes), jnp.float32),
                    pltpu.SemaphoreType.DMA((3,)),
                ],
            )
            break
        for way in STAGES[number + 1][0]:
            above = way == "up"
            state, edges[way] = call(
                functools.partial(join_kernel, weights[1], above),
                [whole, edge],
                [VMEM] * 4,
                [coefs, state, halos["down" if above else "up"], phase_map],
                flops=cells * 10,
                aliases={1: 0},
            )
    peaks = lax.all_to_all(peak, ("gx", "gy"), 0, 0, tiled=True)
    (largest,) = call(peak_kernel, [shaped(1, 1)], [VMEM], [peaks], flops=1000)
    return (advanced, jnp.reshape(largest, (1,)))


def solution(mesh):
    return jax.shard_map(
        advance,
        mesh=mesh,
        in_specs=(P(None, "gx", "gy", None), P("gx", "gy", None), P(), P()),
        out_specs=(P(None, "gx", "gy", None), P()),
        check_vma=False,
    )
```

```python
import functools
import math

import jax
import jax.numpy as jnp
from jax import lax
from jax.experimental import pallas as pl
from jax.experimental.pallas import tpu as pltpu
from jax.sharding import PartitionSpec as P


PERIOD = 64


gamma_air = 1.4
gamma_water = 4.4
pinf_water = 3.0
cfl_number = 0.9
gravity = 1.0
shake_amp = 0.8
two_pi = 2.0 * math.pi
coef_one = 0.75
coef_two = -0.15
coef_three = 1.0 / 60.0
one_third = 1.0 / 3.0
two_thirds = 2.0 / 3.0

STAGES = (
    (("up", "down"), (0.0, 1.0)),
    (("down", "up"), (0.75, 0.25)),
    (("up", "down"), (one_third, two_thirds)),
)
WIDTH = 3
TILE = 8
VMEM = pl.BlockSpec(memory_space=pltpu.VMEM)
HBM = pl.BlockSpec(memory_space=pltpu.HBM)


def point(state, phase):
    density, one, two, three, energy = state
    water_frac = phase.astype(jnp.float32)
    gamma_cell = gamma_air + (gamma_water - gamma_air) * water_frac
    pinf_cell = pinf_water * water_frac
    inverse = 1.0 / density
    velocity = (one * inverse, two * inverse, three * inverse)
    kinetic = 0.5 * (one * velocity[0] + two * velocity[1] + three * velocity[2])
    press_now = (gamma_cell - 1.0) * (energy - kinetic) - gamma_cell * pinf_cell
    return velocity, press_now, inverse, gamma_cell, pinf_cell


def flux(state, velocity, press_now, direction):
    speed = velocity[direction]
    pieces = [state[1 + direction]]
    for member in range(3):
        moment = state[1 + member] * speed
        pieces.append(moment + press_now if member == direction else moment)
    pieces.append((state[4] + press_now) * speed)
    return pieces


def plane(ref, index):
    return [ref[member, index] for member in range(5)]


def edge_kernel(state_ref, phase_ref, last_ref, leading_ref, planes, phases, semaphores):
    length = state_ref.shape[1]
    sides = ((last_ref, length - WIDTH), (leading_ref, 0))
    copies = []
    for side, (_, start) in enumerate(sides):
        near = pl.ds(start, WIDTH)
        copies.append(pltpu.make_async_copy(state_ref.at[:, near], planes.at[side], semaphores.at[2 * side]))
        copies.append(pltpu.make_async_copy(phase_ref.at[near], phases.at[side], semaphores.at[2 * side + 1]))
    for copy in copies:
        copy.start()
    for side, (target, _) in enumerate(sides):
        copies[2 * side].wait()
        copies[2 * side + 1].wait()
        for k in range(WIDTH):
            state = [planes[side, member, k] for member in range(5)]
            velocity, press_now, *_ = point(state, phases[side, k])
            for member, piece in enumerate(flux(state, velocity, press_now, 0)):
                target[member, k] = piece


def rows_kernel(state_ref, phase_ref, rows_ref):
    rows = state_ref.shape[2]
    below = lax.broadcasted_iota(jnp.int32, (TILE, state_ref.shape[3]), 0) < TILE // 2

    def body(index, carry):
        state = []
        for member in range(5):
            first = state_ref[member, index, 0:TILE]
            final = state_ref[member, index, rows - TILE : rows]
            state.append(jnp.where(below, first, final))
        phase = jnp.where(below, phase_ref[index, 0:TILE], phase_ref[index, rows - TILE : rows])
        velocity, press_now, *_ = point(state, phase)
        for member, piece in enumerate(flux(state, velocity, press_now, 1)):
            rows_ref[member, index] = piece
        return carry

    lax.fori_loop(0, state_ref.shape[1], body, 0, unroll=2)


def middle_kernel(weights, first, coefs, state_ref, phase_ref, start_ref, out_ref, xs, ys, zs):
    length, rows, lanes = phase_ref.shape
    blank = jnp.zeros((rows, lanes), jnp.float32)
    for member in range(5):
        for k in range(WIDTH):
            xs[member, k] = blank
            xs[member, WIDTH + length + k] = blank

    def fill(index, carry):
        state = plane(state_ref, index)
        velocity, press_now, *_ = point(state, phase_ref[index])
        for member, piece in enumerate(flux(state, velocity, press_now, 0)):
            xs[member, WIDTH + index] = piece
        for member, piece in enumerate(flux(state, velocity, press_now, 1)):
            ys[member, index, TILE : TILE + rows] = piece
            ys[member, index, 0:TILE] = blank[0:TILE]
            ys[member, index, TILE + rows : TILE + rows + TILE] = blank[0:TILE]
        for member, piece in enumerate(flux(state, velocity, press_now, 2)):
            zs[member, index] = piece
        return carry

    lax.fori_loop(0, length, fill, 0, unroll=2)
    keep, share = weights
    steps = [coefs[k] * share for k in range(3)]
    source = coefs[3] * share

    def update(index, carry):
        for member in range(5):
            third = zs[member, index]
            total = None
            for k in range(1, WIDTH + 1):
                ahead = xs[member, WIDTH + index + k] - xs[member, WIDTH + index - k]
                ahead = ahead + (
                    ys[member, index, TILE + k : TILE + k + rows] - ys[member, index, TILE - k : TILE - k + rows]
                )
                ahead = ahead + (pltpu.roll(third, lanes - k, 1) - pltpu.roll(third, k, 1))
                term = steps[k - 1] * ahead
                total = term if total is None else total + term
            value = state_ref[member, index]
            if first:
                value = value - total
            else:
                value = keep * start_ref[member, index] + (share * value - total)
            if member == 3:
                value = value + source * state_ref[0, index]
            if member == 4:
                value = value + source * state_ref[3, index]
            out_ref[member, index] = value
        return carry

    lax.fori_loop(0, length, update, 0, unroll=4)


def border_kernel(share, final, coefs, partial_ref, phase_ref, before_ref, after_ref, out_ref, *inner_ref):
    _, length, rows, lanes = partial_ref.shape
    place = lax.broadcasted_iota(jnp.int32, (TILE, lanes), 0)
    blank = jnp.zeros((TILE, lanes), jnp.float32)
    steps = [coefs[k, 0:TILE] * share for k in range(3)]
    early = [jnp.where(place < k, steps[k - 1], blank) for k in range(1, WIDTH + 1)]
    late = [jnp.where(place >= TILE - k, steps[k - 1], blank) for k in range(1, WIDTH + 1)]

    def border(index, carry):
        for member in range(5):
            before, after = before_ref[member, index], after_ref[member, index]
            first = partial_ref[member, index, 0:TILE]
            final = partial_ref[member, index, rows - TILE : rows]
            for k in range(1, WIDTH + 1):
                first = first + early[k - 1] * pltpu.roll(before, k, 0)
                final = final - late[k - 1] * pltpu.roll(after, TILE - k, 0)
            out_ref[member, index, 0:TILE] = first
            out_ref[member, index, rows - TILE : rows] = final
        return carry

    lax.fori_loop(0, length, border, 0, unroll=2)
    if final:

        def fastest(index, largest):
            return jnp.maximum(largest, wave_speed(plane(out_ref, index), phase_ref[index]))

        blank = jnp.zeros((rows, lanes), jnp.float32)
        inner_ref[0][...] = lax.fori_loop(WIDTH, length - WIDTH, fastest, blank, unroll=2)


def with_halo(share, coefs, partial_ref, halo_ref, above):
    length = partial_ref.shape[1]
    steps = [coefs[k] * (-share if above else share) for k in range(3)]
    for near in range(WIDTH):
        index = length - 1 - near if above else near
        state = plane(partial_ref, index)
        for k in range(near + 1, WIDTH + 1):
            place = k - 1 - near if above else WIDTH + near - k
            state = [value + steps[k - 1] * halo_ref[member, place] for member, value in enumerate(state)]
        yield index, WIDTH - 1 - near if above else near, state


def join_kernel(share, above, coefs, partial_ref, halo_ref, phase_ref, out_ref, edge_ref):
    for index, place, state in with_halo(share, coefs, partial_ref, halo_ref, above):
        velocity, press_now, *_ = point(state, phase_ref[index])
        for member, piece in enumerate(flux(state, velocity, press_now, 0)):
            edge_ref[member, place] = piece
        for member in range(5):
            out_ref[member, index] = state[member]


def wave_speed(state, phase):
    velocity, press_now, inverse, gamma_cell, pinf_cell = point(state, phase)
    speed = jnp.abs(velocity[0]) + jnp.abs(velocity[1]) + jnp.abs(velocity[2])
    return speed + 3.0 * jnp.sqrt(gamma_cell * (press_now + pinf_cell) * inverse)


def final_kernel(share, coefs, partial_ref, left_ref, right_ref, phase_ref, inner_ref, out_ref, peak_ref):
    largest = inner_ref[...]
    for halo_ref, above in ((left_ref, False), (right_ref, True)):
        for index, place, state in with_halo(share, coefs, partial_ref, halo_ref, above):
            for member in range(5):
                out_ref[member, index] = state[member]
            largest = jnp.maximum(largest, wave_speed(state, phase_ref[index]))
    largest = jnp.max(largest, axis=0, keepdims=True)
    peak_ref[...] = jnp.broadcast_to(largest, peak_ref.shape)


def output_kernel(state_ref, peaks_ref, advanced_ref, largest_ref, peak, semaphores):
    whole = pltpu.make_async_copy(state_ref, advanced_ref, semaphores.at[0])
    whole.start()
    largest = jnp.max(jnp.max(peaks_ref[...], axis=0, keepdims=True), axis=1, keepdims=True)
    peak[...] = jnp.broadcast_to(largest, peak.shape)
    single = pltpu.make_async_copy(peak, largest_ref, semaphores.at[1])
    single.start()
    whole.wait()
    single.wait()


def shaped(*shape):
    return jax.ShapeDtypeStruct(shape, jnp.float32)


def call(kernel, outs, specs, args, *, flops, scratch=(), aliases=None, places=None):
    moved = 4 * sum(math.prod(o.shape) for o in outs)
    return pl.pallas_call(
        kernel,
        out_shape=list(outs),
        in_specs=specs,
        out_specs=places or [VMEM] * len(outs),
        scratch_shapes=list(scratch),
        input_output_aliases=aliases or {},
        cost_estimate=pl.CostEstimate(flops=flops, bytes_accessed=moved, transcendentals=0),
        compiler_params=pltpu.CompilerParams(vmem_limit_bytes=16 << 20),
    )(*args)


def advance(fields, phase_map, lagged_speed, step_count):
    _, length, rows, lanes = fields.shape
    cells = length * rows * lanes
    time_step = cfl_number / lagged_speed[0]
    gravity_now = gravity * (
        1.0 + shake_amp * jnp.cos(two_pi * step_count[0].astype(jnp.float32) / PERIOD)
    )
    coefs = time_step * jnp.stack(
        [jnp.float32(coef_one), jnp.float32(coef_two), jnp.float32(coef_three), gravity_now]
    )
    coefs = jnp.broadcast_to(coefs[:, None, None], (4, rows, lanes))
    along, across = lax.axis_size("gx"), lax.axis_size("gy")
    up = [(i, (i + 1) % along) for i in range(along)]
    down = [(j, i) for i, j in up]
    over = [(i, (i + 1) % across) for i in range(across)]
    back = [(j, i) for i, j in over]
    edge = shaped(5, WIDTH, rows, lanes)
    whole = shaped(5, length, rows, lanes)
    row_tile = shaped(5, length, TILE, lanes)

    state = fields
    last, leading = call(
        edge_kernel,
        [edge, edge],
        [HBM, HBM],
        [pltpu.with_memory_space_constraint(array, pltpu.HBM) for array in (state, phase_map)],
        flops=cells * 20,
        scratch=[
            pltpu.VMEM((2, 5, WIDTH, rows, lanes), jnp.float32),
            pltpu.VMEM((2, WIDTH, rows, lanes), jnp.int32),
            pltpu.SemaphoreType.DMA((4,)),
        ],
    )
    edges = {"up": last, "down": leading}
    for number, ((first, second), weights) in enumerate(STAGES):
        halos = {}
        for way in (first, second):
            halos[way] = lax.ppermute(edges[way], "gx", up if way == "up" else down)
        (sent,) = call(rows_kernel, [row_tile], [VMEM, VMEM], [state, phase_map], flops=cells * 10)
        before = lax.ppermute(sent, "gy", over)
        after = before if across == 2 else lax.ppermute(sent, "gy", back)
        final = number == len(STAGES) - 1
        (state,) = call(
            functools.partial(middle_kernel, weights, number == 0),
            [whole],
            [VMEM] * 4,
            [coefs, state, phase_map, fields],
            flops=cells * 1000,
            scratch=[
                pltpu.VMEM((5, length + 2 * WIDTH, rows, lanes), jnp.float32),
                pltpu.VMEM((5, length, rows + 2 * TILE, lanes), jnp.float32),
                pltpu.VMEM((5, length, rows, lanes), jnp.float32),
            ],
        )
        state, *inner = call(
            functools.partial(border_kernel, weights[1], final),
            [whole, shaped(rows, lanes)] if final else [whole],
            [VMEM] * 5,
            [coefs, state, phase_map, before, after],
            flops=cells * 20,
            aliases={1: 0},
        )
        if final:
            state, peak = call(
                functools.partial(final_kernel, weights[1]),
                [whole, shaped(along * across, lanes)],
                [VMEM] * 6,
                [coefs, state, halos["up"], halos["down"], phase_map, *inner],
                flops=cells * 50,
                aliases={1: 0},
            )
            break
        for way in STAGES[number + 1][0]:
            above = way == "up"
            state, edges[way] = call(
                functools.partial(join_kernel, weights[1], above),
                [whole, edge],
                [VMEM] * 4,
                [coefs, state, halos["down" if above else "up"], phase_map],
                flops=cells * 10,
                aliases={1: 0},
            )
    peaks = lax.all_to_all(peak, ("gx", "gy"), 0, 0, tiled=True)
    advanced, largest = call(
        output_kernel,
        [whole, shaped(1, lanes)],
        [VMEM, VMEM],
        [state, peaks],
        flops=1000,
        places=[HBM, HBM],
        scratch=[pltpu.VMEM((1, lanes), jnp.float32), pltpu.SemaphoreType.DMA((2,))],
    )
    return (advanced, largest[0, 0:1])


def solution(mesh):
    return jax.shard_map(
        advance,
        mesh=mesh,
        in_specs=(P(None, "gx", "gy", None), P("gx", "gy", None), P(), P()),
        out_specs=(P(None, "gx", "gy", None), P()),
        check_vma=False,
    )
```

```python
import functools
import math

import jax
import jax.numpy as jnp
from jax import lax
from jax.experimental import pallas as pl
from jax.experimental.pallas import tpu as pltpu
from jax.sharding import PartitionSpec as P


PERIOD = 64


gamma_air = 1.4
gamma_water = 4.4
pinf_water = 3.0
cfl_number = 0.9
gravity = 1.0
shake_amp = 0.8
two_pi = 2.0 * math.pi
coef_one = 0.75
coef_two = -0.15
coef_three = 1.0 / 60.0
one_third = 1.0 / 3.0
two_thirds = 2.0 / 3.0

STAGES = (
    (("up", "down"), (0.0, 1.0)),
    (("down", "up"), (0.75, 0.25)),
    (("up", "down"), (one_third, two_thirds)),
)
WIDTH = 3
TILE = 8
VMEM = pl.BlockSpec(memory_space=pltpu.VMEM)
HBM = pl.BlockSpec(memory_space=pltpu.HBM)


def point(state, phase):
    density, one, two, three, energy = state
    water_frac = phase.astype(jnp.float32)
    gamma_cell = gamma_air + (gamma_water - gamma_air) * water_frac
    pinf_cell = pinf_water * water_frac
    inverse = 1.0 / density
    velocity = (one * inverse, two * inverse, three * inverse)
    kinetic = 0.5 * (one * velocity[0] + two * velocity[1] + three * velocity[2])
    press_now = (gamma_cell - 1.0) * (energy - kinetic) - gamma_cell * pinf_cell
    return velocity, press_now, inverse, gamma_cell, pinf_cell


def flux(state, velocity, press_now, direction):
    speed = velocity[direction]
    pieces = [state[1 + direction]]
    for member in range(3):
        moment = state[1 + member] * speed
        pieces.append(moment + press_now if member == direction else moment)
    pieces.append((state[4] + press_now) * speed)
    return pieces


def plane(ref, index):
    return [ref[member, index] for member in range(5)]


def edge_kernel(state_ref, phase_ref, last_ref, leading_ref, planes, phases, semaphores):
    length = state_ref.shape[1]
    sides = ((last_ref, length - WIDTH), (leading_ref, 0))
    copies = []
    for side, (_, start) in enumerate(sides):
        near = pl.ds(start, WIDTH)
        copies.append(pltpu.make_async_copy(state_ref.at[:, near], planes.at[side], semaphores.at[2 * side]))
        copies.append(pltpu.make_async_copy(phase_ref.at[near], phases.at[side], semaphores.at[2 * side + 1]))
    for copy in copies:
        copy.start()
    for side, (target, _) in enumerate(sides):
        copies[2 * side].wait()
        copies[2 * side + 1].wait()
        for k in range(WIDTH):
            state = [planes[side, member, k] for member in range(5)]
            velocity, press_now, *_ = point(state, phases[side, k])
            for member, piece in enumerate(flux(state, velocity, press_now, 0)):
                target[member, k] = piece


def rows_kernel(state_ref, phase_ref, rows_ref):
    rows = state_ref.shape[2]
    below = lax.broadcasted_iota(jnp.int32, (TILE, state_ref.shape[3]), 0) < TILE // 2

    def body(index, carry):
        state = []
        for member in range(5):
            first = state_ref[member, index, 0:TILE]
            final = state_ref[member, index, rows - TILE : rows]
            state.append(jnp.where(below, first, final))
        phase = jnp.where(below, phase_ref[index, 0:TILE], phase_ref[index, rows - TILE : rows])
        velocity, press_now, *_ = point(state, phase)
        for member, piece in enumerate(flux(state, velocity, press_now, 1)):
            rows_ref[member, index] = piece
        return carry

    lax.fori_loop(0, state_ref.shape[1], body, 0, unroll=2)


def middle_kernel(weights, first, coefs, state_ref, phase_ref, start_ref, out_ref, xs, ys, zs):
    length, rows, lanes = phase_ref.shape
    blank = jnp.zeros((rows, lanes), jnp.float32)
    for member in range(5):
        for k in range(WIDTH):
            xs[member, k] = blank
            xs[member, WIDTH + length + k] = blank

    def fill(index, carry):
        state = plane(state_ref, index)
        velocity, press_now, *_ = point(state, phase_ref[index])
        for member, piece in enumerate(flux(state, velocity, press_now, 0)):
            xs[member, WIDTH + index] = piece
        for member, piece in enumerate(flux(state, velocity, press_now, 1)):
            ys[member, index, TILE : TILE + rows] = piece
            ys[member, index, 0:TILE] = blank[0:TILE]
            ys[member, index, TILE + rows : TILE + rows + TILE] = blank[0:TILE]
        for member, piece in enumerate(flux(state, velocity, press_now, 2)):
            zs[member, index] = piece
        return carry

    lax.fori_loop(0, length, fill, 0, unroll=4)
    keep, share = weights
    steps = [coefs[k] * share for k in range(3)]
    source = coefs[3] * share

    def update(index, carry):
        for member in range(5):
            third = zs[member, index]
            total = None
            for k in range(1, WIDTH + 1):
                ahead = xs[member, WIDTH + index + k] - xs[member, WIDTH + index - k]
                ahead = ahead + (
                    ys[member, index, TILE + k : TILE + k + rows] - ys[member, index, TILE - k : TILE - k + rows]
                )
                ahead = ahead + (pltpu.roll(third, lanes - k, 1) - pltpu.roll(third, k, 1))
                term = steps[k - 1] * ahead
                total = term if total is None else total + term
            value = state_ref[member, index]
            if first:
                value = value - total
            else:
                value = keep * start_ref[member, index] + (share * value - total)
            if member == 3:
                value = value + source * state_ref[0, index]
            if member == 4:
                value = value + source * state_ref[3, index]
            out_ref[member, index] = value
        return carry

    lax.fori_loop(0, length, update, 0, unroll=6)


def border_kernel(share, final, coefs, partial_ref, phase_ref, before_ref, after_ref, out_ref, *rest):
    _, length, rows, lanes = partial_ref.shape
    place = lax.broadcasted_iota(jnp.int32, (TILE, lanes), 0)
    blank = jnp.zeros((TILE, lanes), jnp.float32)
    steps = [coefs[k, 0:TILE] * share for k in range(3)]
    early = [jnp.where(place < k, steps[k - 1], blank) for k in range(1, WIDTH + 1)]
    late = [jnp.where(place >= TILE - k, steps[k - 1], blank) for k in range(1, WIDTH + 1)]

    def border(index, carry):
        for member in range(5):
            before, after = before_ref[member, index], after_ref[member, index]
            first = partial_ref[member, index, 0:TILE]
            final = partial_ref[member, index, rows - TILE : rows]
            for k in range(1, WIDTH + 1):
                first = first + early[k - 1] * pltpu.roll(before, k, 0)
                final = final - late[k - 1] * pltpu.roll(after, TILE - k, 0)
            out_ref[member, index, 0:TILE] = first
            out_ref[member, index, rows - TILE : rows] = final
        return carry

    lax.fori_loop(0, length, border, 0, unroll=4)
    if final:
        inner_ref, advanced_ref, semaphore = rest
        inner = pl.ds(WIDTH, length - 2 * WIDTH)
        copy = pltpu.make_async_copy(out_ref.at[:, inner], advanced_ref.at[:, inner], semaphore)
        copy.start()

        def fastest(index, largest):
            return jnp.maximum(largest, wave_speed(plane(out_ref, index), phase_ref[index]))

        blank = jnp.zeros((rows, lanes), jnp.float32)
        inner_ref[...] = lax.fori_loop(WIDTH, length - WIDTH, fastest, blank, unroll=3)
        copy.wait()


def with_halo(share, coefs, partial_ref, halo_ref, above):
    length = partial_ref.shape[1]
    steps = [coefs[k] * (-share if above else share) for k in range(3)]
    for near in range(WIDTH):
        index = length - 1 - near if above else near
        state = plane(partial_ref, index)
        for k in range(near + 1, WIDTH + 1):
            place = k - 1 - near if above else WIDTH + near - k
            state = [value + steps[k - 1] * halo_ref[member, place] for member, value in enumerate(state)]
        yield index, WIDTH - 1 - near if above else near, state


def join_kernel(share, above, coefs, partial_ref, halo_ref, phase_ref, out_ref, edge_ref):
    for index, place, state in with_halo(share, coefs, partial_ref, halo_ref, above):
        velocity, press_now, *_ = point(state, phase_ref[index])
        for member, piece in enumerate(flux(state, velocity, press_now, 0)):
            edge_ref[member, place] = piece
        for member in range(5):
            out_ref[member, index] = state[member]


def wave_speed(state, phase):
    velocity, press_now, inverse, gamma_cell, pinf_cell = point(state, phase)
    speed = jnp.abs(velocity[0]) + jnp.abs(velocity[1]) + jnp.abs(velocity[2])
    return speed + 3.0 * jnp.sqrt(gamma_cell * (press_now + pinf_cell) * inverse)


def final_kernel(share, coefs, partial_ref, left_ref, right_ref, phase_ref, inner_ref, out_ref, peak_ref):
    largest = inner_ref[...]
    for halo_ref, above in ((left_ref, False), (right_ref, True)):
        for index, place, state in with_halo(share, coefs, partial_ref, halo_ref, above):
            for member in range(5):
                out_ref[member, index] = state[member]
            largest = jnp.maximum(largest, wave_speed(state, phase_ref[index]))
    largest = jnp.max(largest, axis=0, keepdims=True)
    peak_ref[...] = jnp.broadcast_to(largest, peak_ref.shape)


def output_kernel(state_ref, peaks_ref, inner_ref, advanced_ref, largest_ref, peak, semaphores):
    length = state_ref.shape[1]
    copies = []
    for side, start in enumerate((0, length - WIDTH)):
        near = pl.ds(start, WIDTH)
        copies.append(pltpu.make_async_copy(state_ref.at[:, near], advanced_ref.at[:, near], semaphores.at[side]))
        copies[side].start()
    largest = jnp.max(jnp.max(peaks_ref[...], axis=0, keepdims=True), axis=1, keepdims=True)
    peak[...] = jnp.broadcast_to(largest, peak.shape)
    copies.append(pltpu.make_async_copy(peak, largest_ref, semaphores.at[2]))
    copies[2].start()
    for copy in copies:
        copy.wait()


def shaped(*shape):
    return jax.ShapeDtypeStruct(shape, jnp.float32)


def call(kernel, outs, specs, args, *, flops, scratch=(), aliases=None, places=None):
    moved = 4 * sum(math.prod(o.shape) for o in outs)
    return pl.pallas_call(
        kernel,
        out_shape=list(outs),
        in_specs=specs,
        out_specs=places or [VMEM] * len(outs),
        scratch_shapes=list(scratch),
        input_output_aliases=aliases or {},
        cost_estimate=pl.CostEstimate(flops=flops, bytes_accessed=moved, transcendentals=0),
        compiler_params=pltpu.CompilerParams(vmem_limit_bytes=16 << 20),
    )(*args)


def advance(fields, phase_map, lagged_speed, step_count):
    _, length, rows, lanes = fields.shape
    cells = length * rows * lanes
    time_step = cfl_number / lagged_speed[0]
    gravity_now = gravity * (
        1.0 + shake_amp * jnp.cos(two_pi * step_count[0].astype(jnp.float32) / PERIOD)
    )
    coefs = time_step * jnp.stack(
        [jnp.float32(coef_one), jnp.float32(coef_two), jnp.float32(coef_three), gravity_now]
    )
    coefs = jnp.broadcast_to(coefs[:, None, None], (4, rows, lanes))
    along, across = lax.axis_size("gx"), lax.axis_size("gy")
    up = [(i, (i + 1) % along) for i in range(along)]
    down = [(j, i) for i, j in up]
    over = [(i, (i + 1) % across) for i in range(across)]
    back = [(j, i) for i, j in over]
    edge = shaped(5, WIDTH, rows, lanes)
    whole = shaped(5, length, rows, lanes)
    row_tile = shaped(5, length, TILE, lanes)

    state = fields
    last, leading = call(
        edge_kernel,
        [edge, edge],
        [HBM, HBM],
        [pltpu.with_memory_space_constraint(array, pltpu.HBM) for array in (state, phase_map)],
        flops=cells * 20,
        scratch=[
            pltpu.VMEM((2, 5, WIDTH, rows, lanes), jnp.float32),
            pltpu.VMEM((2, WIDTH, rows, lanes), jnp.int32),
            pltpu.SemaphoreType.DMA((4,)),
        ],
    )
    edges = {"up": last, "down": leading}
    for number, ((first, second), weights) in enumerate(STAGES):
        halos = {}
        for way in (first, second):
            halos[way] = lax.ppermute(edges[way], "gx", up if way == "up" else down)
        (sent,) = call(rows_kernel, [row_tile], [VMEM, VMEM], [state, phase_map], flops=cells * 10)
        before = lax.ppermute(sent, "gy", over)
        after = before if across == 2 else lax.ppermute(sent, "gy", back)
        final = number == len(STAGES) - 1
        (state,) = call(
            functools.partial(middle_kernel, weights, number == 0),
            [whole],
            [VMEM] * 4,
            [coefs, state, phase_map, fields],
            flops=cells * 1000,
            scratch=[
                pltpu.VMEM((5, length + 2 * WIDTH, rows, lanes), jnp.float32),
                pltpu.VMEM((5, length, rows + 2 * TILE, lanes), jnp.float32),
                pltpu.VMEM((5, length, rows, lanes), jnp.float32),
            ],
        )
        state, *inner = call(
            functools.partial(border_kernel, weights[1], final),
            [whole, shaped(rows, lanes), whole] if final else [whole],
            [VMEM] * 5,
            [coefs, state, phase_map, before, after],
            flops=cells * 20,
            aliases={1: 0},
            places=[VMEM, VMEM, HBM] if final else None,
            scratch=[pltpu.SemaphoreType.DMA] if final else (),
        )
        if final:
            state, peak = call(
                functools.partial(final_kernel, weights[1]),
                [whole, shaped(along * across, lanes)],
                [VMEM] * 6,
                [coefs, state, halos["up"], halos["down"], phase_map, inner[0]],
                flops=cells * 50,
                aliases={1: 0},
            )
            break
        for way in STAGES[number + 1][0]:
            above = way == "up"
            state, edges[way] = call(
                functools.partial(join_kernel, weights[1], above),
                [whole, edge],
                [VMEM] * 4,
                [coefs, state, halos["down" if above else "up"], phase_map],
                flops=cells * 10,
                aliases={1: 0},
            )
    peaks = lax.all_to_all(peak, ("gx", "gy"), 0, 0, tiled=True)
    advanced, largest = call(
        output_kernel,
        [whole, shaped(1, lanes)],
        [VMEM, VMEM, HBM],
        [state, peaks, inner[1]],
        flops=1000,
        places=[HBM, HBM],
        scratch=[pltpu.VMEM((1, lanes), jnp.float32), pltpu.SemaphoreType.DMA((3,))],
        aliases={2: 0},
    )
    return (advanced, largest[0, 0:1])


def solution(mesh):
    return jax.shard_map(
        advance,
        mesh=mesh,
        in_specs=(P(None, "gx", "gy", None), P("gx", "gy", None), P(), P()),
        out_specs=(P(None, "gx", "gy", None), P()),
        check_vma=False,
    )
```

```python
import functools
import math

import jax
import jax.numpy as jnp
from jax import lax
from jax.experimental import pallas as pl
from jax.experimental.pallas import tpu as pltpu
from jax.sharding import PartitionSpec as P


PERIOD = 64


gamma_air = 1.4
gamma_water = 4.4
pinf_water = 3.0
cfl_number = 0.9
gravity = 1.0
shake_amp = 0.8
two_pi = 2.0 * math.pi
coef_one = 0.75
coef_two = -0.15
coef_three = 1.0 / 60.0
one_third = 1.0 / 3.0
two_thirds = 2.0 / 3.0

STAGES = (
    (("up", "down"), (0.0, 1.0)),
    (("down", "up"), (0.75, 0.25)),
    (("up", "down"), (one_third, two_thirds)),
)
WIDTH = 3
TILE = 8
VMEM = pl.BlockSpec(memory_space=pltpu.VMEM)
HBM = pl.BlockSpec(memory_space=pltpu.HBM)


def point(state, phase):
    density, one, two, three, energy = state
    water_frac = phase.astype(jnp.float32)
    gamma_cell = gamma_air + (gamma_water - gamma_air) * water_frac
    pinf_cell = pinf_water * water_frac
    inverse = 1.0 / density
    velocity = (one * inverse, two * inverse, three * inverse)
    kinetic = 0.5 * (one * velocity[0] + two * velocity[1] + three * velocity[2])
    press_now = (gamma_cell - 1.0) * (energy - kinetic) - gamma_cell * pinf_cell
    return velocity, press_now, inverse, gamma_cell, pinf_cell


def flux(state, velocity, press_now, direction):
    speed = velocity[direction]
    pieces = [state[1 + direction]]
    for member in range(3):
        moment = state[1 + member] * speed
        pieces.append(moment + press_now if member == direction else moment)
    pieces.append((state[4] + press_now) * speed)
    return pieces


def plane(ref, index):
    return [ref[member, index] for member in range(5)]


def edge_kernel(state_ref, phase_ref, last_ref, leading_ref, planes, phases, semaphores):
    length = state_ref.shape[1]
    sides = ((last_ref, length - WIDTH), (leading_ref, 0))
    copies = []
    for side, (_, start) in enumerate(sides):
        near = pl.ds(start, WIDTH)
        copies.append(pltpu.make_async_copy(state_ref.at[:, near], planes.at[side], semaphores.at[2 * side]))
        copies.append(pltpu.make_async_copy(phase_ref.at[near], phases.at[side], semaphores.at[2 * side + 1]))
    for copy in copies:
        copy.start()
    for side, (target, _) in enumerate(sides):
        copies[2 * side].wait()
        copies[2 * side + 1].wait()
        for k in range(WIDTH):
            state = [planes[side, member, k] for member in range(5)]
            velocity, press_now, *_ = point(state, phases[side, k])
            for member, piece in enumerate(flux(state, velocity, press_now, 0)):
                target[member, k] = piece


def rows_kernel(state_ref, phase_ref, rows_ref):
    rows = state_ref.shape[2]
    below = lax.broadcasted_iota(jnp.int32, (TILE, state_ref.shape[3]), 0) < TILE // 2

    def body(index, carry):
        state = []
        for member in range(5):
            first = state_ref[member, index, 0:TILE]
            final = state_ref[member, index, rows - TILE : rows]
            state.append(jnp.where(below, first, final))
        phase = jnp.where(below, phase_ref[index, 0:TILE], phase_ref[index, rows - TILE : rows])
        velocity, press_now, *_ = point(state, phase)
        for member, piece in enumerate(flux(state, velocity, press_now, 1)):
            rows_ref[member, index] = piece
        return carry

    lax.fori_loop(0, state_ref.shape[1], body, 0, unroll=2)


def middle_kernel(weights, first, coefs, state_ref, phase_ref, start_ref, out_ref, xs, ys, zs):
    length, rows, lanes = phase_ref.shape
    blank = jnp.zeros((rows, lanes), jnp.float32)
    for member in range(5):
        for k in range(WIDTH):
            xs[member, k] = blank
            xs[member, WIDTH + length + k] = blank

    def fill(index, carry):
        state = plane(state_ref, index)
        velocity, press_now, *_ = point(state, phase_ref[index])
        for member, piece in enumerate(flux(state, velocity, press_now, 0)):
            xs[member, WIDTH + index] = piece
        for member, piece in enumerate(flux(state, velocity, press_now, 1)):
            ys[member, index, TILE : TILE + rows] = piece
            ys[member, index, 0:TILE] = blank[0:TILE]
            ys[member, index, TILE + rows : TILE + rows + TILE] = blank[0:TILE]
        for member, piece in enumerate(flux(state, velocity, press_now, 2)):
            zs[member, index] = piece
        return carry

    lax.fori_loop(0, length, fill, 0, unroll=4)
    keep, share = weights
    steps = [coefs[k] * share for k in range(3)]
    source = coefs[3] * share

    def update(index, carry):
        for member in range(5):
            third = zs[member, index]
            total = None
            for k in range(1, WIDTH + 1):
                ahead = xs[member, WIDTH + index + k] - xs[member, WIDTH + index - k]
                ahead = ahead + (
                    ys[member, index, TILE + k : TILE + k + rows] - ys[member, index, TILE - k : TILE - k + rows]
                )
                ahead = ahead + (pltpu.roll(third, lanes - k, 1) - pltpu.roll(third, k, 1))
                term = steps[k - 1] * ahead
                total = term if total is None else total + term
            value = state_ref[member, index]
            if first:
                value = value - total
            else:
                value = keep * start_ref[member, index] + (share * value - total)
            if member == 3:
                value = value + source * state_ref[0, index]
            if member == 4:
                value = value + source * state_ref[3, index]
            out_ref[member, index] = value
        return carry

    lax.fori_loop(0, length, update, 0, unroll=6)


def border_kernel(share, final, coefs, partial_ref, phase_ref, before_ref, after_ref, out_ref, *rest):
    _, length, rows, lanes = partial_ref.shape
    place = lax.broadcasted_iota(jnp.int32, (TILE, lanes), 0)
    blank = jnp.zeros((TILE, lanes), jnp.float32)
    steps = [coefs[k, 0:TILE] * share for k in range(3)]
    early = [jnp.where(place < k, steps[k - 1], blank) for k in range(1, WIDTH + 1)]
    late = [jnp.where(place >= TILE - k, steps[k - 1], blank) for k in range(1, WIDTH + 1)]

    def border(index, carry):
        for member in range(5):
            before, after = before_ref[member, index], after_ref[member, index]
            first = partial_ref[member, index, 0:TILE]
            final = partial_ref[member, index, rows - TILE : rows]
            for k in range(1, WIDTH + 1):
                first = first + early[k - 1] * pltpu.roll(before, k, 0)
                final = final - late[k - 1] * pltpu.roll(after, TILE - k, 0)
            out_ref[member, index, 0:TILE] = first
            out_ref[member, index, rows - TILE : rows] = final
        return carry

    lax.fori_loop(0, length, border, 0, unroll=4)
    if final:
        inner_ref, advanced_ref, semaphore = rest
        inner = pl.ds(WIDTH, length - 2 * WIDTH)
        copy = pltpu.make_async_copy(out_ref.at[:, inner], advanced_ref.at[:, inner], semaphore)
        copy.start()

        def fastest(index, largest):
            return jnp.maximum(largest, wave_speed(plane(out_ref, index), phase_ref[index]))

        blank = jnp.zeros((rows, lanes), jnp.float32)
        inner_ref[...] = lax.fori_loop(WIDTH, length - WIDTH, fastest, blank, unroll=3)
        copy.wait()


def with_halo(share, coefs, partial_ref, halo_ref, above):
    length = partial_ref.shape[1]
    steps = [coefs[k] * (-share if above else share) for k in range(3)]
    for near in range(WIDTH):
        index = length - 1 - near if above else near
        state = plane(partial_ref, index)
        for k in range(near + 1, WIDTH + 1):
            place = k - 1 - near if above else WIDTH + near - k
            state = [value + steps[k - 1] * halo_ref[member, place] for member, value in enumerate(state)]
        yield index, WIDTH - 1 - near if above else near, state


def join_kernel(share, above, coefs, partial_ref, halo_ref, phase_ref, out_ref, edge_ref):
    for index, place, state in with_halo(share, coefs, partial_ref, halo_ref, above):
        velocity, press_now, *_ = point(state, phase_ref[index])
        for member, piece in enumerate(flux(state, velocity, press_now, 0)):
            edge_ref[member, place] = piece
        for member in range(5):
            out_ref[member, index] = state[member]


def wave_speed(state, phase):
    velocity, press_now, inverse, gamma_cell, pinf_cell = point(state, phase)
    speed = jnp.abs(velocity[0]) + jnp.abs(velocity[1]) + jnp.abs(velocity[2])
    return speed + 3.0 * jnp.sqrt(gamma_cell * (press_now + pinf_cell) * inverse)


def final_kernel(share, coefs, partial_ref, left_ref, right_ref, phase_ref, inner_ref, out_ref, peak_ref):
    largest = inner_ref[...]
    for halo_ref, above in ((left_ref, False), (right_ref, True)):
        for index, place, state in with_halo(share, coefs, partial_ref, halo_ref, above):
            for member in range(5):
                out_ref[member, index] = state[member]
            largest = jnp.maximum(largest, wave_speed(state, phase_ref[index]))
    largest = jnp.max(largest, axis=0, keepdims=True)
    peak_ref[...] = jnp.broadcast_to(largest, peak_ref.shape)


def output_kernel(state_ref, peaks_ref, inner_ref, advanced_ref, largest_ref, peak, semaphores):
    length = state_ref.shape[1]
    copies = []
    for side, start in enumerate((0, length - WIDTH)):
        near = pl.ds(start, WIDTH)
        copies.append(pltpu.make_async_copy(state_ref.at[:, near], advanced_ref.at[:, near], semaphores.at[side]))
        copies[side].start()
    largest = jnp.max(jnp.max(peaks_ref[...], axis=0, keepdims=True), axis=1, keepdims=True)
    peak[...] = jnp.broadcast_to(largest, peak.shape)
    copies.append(pltpu.make_async_copy(peak, largest_ref, semaphores.at[2]))
    copies[2].start()
    for copy in copies:
        copy.wait()


def shaped(*shape):
    return jax.ShapeDtypeStruct(shape, jnp.float32)


def call(kernel, outs, specs, args, *, flops, scratch=(), aliases=None, places=None):
    moved = 4 * sum(math.prod(o.shape) for o in outs)
    return pl.pallas_call(
        kernel,
        out_shape=list(outs),
        in_specs=specs,
        out_specs=places or [VMEM] * len(outs),
        scratch_shapes=list(scratch),
        input_output_aliases=aliases or {},
        cost_estimate=pl.CostEstimate(flops=flops, bytes_accessed=moved, transcendentals=0),
        compiler_params=pltpu.CompilerParams(vmem_limit_bytes=16 << 20),
    )(*args)


def advance(fields, phase_map, lagged_speed, step_count):
    _, length, rows, lanes = fields.shape
    cells = length * rows * lanes
    time_step = cfl_number / lagged_speed[0]
    gravity_now = gravity * (
        1.0 + shake_amp * jnp.cos(two_pi * step_count[0].astype(jnp.float32) / PERIOD)
    )
    coefs = time_step * jnp.stack(
        [jnp.float32(coef_one), jnp.float32(coef_two), jnp.float32(coef_three), gravity_now]
    )
    coefs = jnp.broadcast_to(coefs[:, None, None], (4, rows, lanes))
    along, across = lax.axis_size("gx"), lax.axis_size("gy")
    up = [(i, (i + 1) % along) for i in range(along)]
    down = [(j, i) for i, j in up]
    over = [(i, (i + 1) % across) for i in range(across)]
    back = [(j, i) for i, j in over]
    edge = shaped(5, WIDTH, rows, lanes)
    whole = shaped(5, length, rows, lanes)
    row_tile = shaped(5, length, TILE, lanes)

    state = fields
    last, leading = call(
        edge_kernel,
        [edge, edge],
        [HBM, HBM],
        [pltpu.with_memory_space_constraint(array, pltpu.HBM) for array in (state, phase_map)],
        flops=cells * 20,
        scratch=[
            pltpu.VMEM((2, 5, WIDTH, rows, lanes), jnp.float32),
            pltpu.VMEM((2, WIDTH, rows, lanes), jnp.int32),
            pltpu.SemaphoreType.DMA((4,)),
        ],
    )
    edges = {"up": last, "down": leading}
    for number, ((first, second), weights) in enumerate(STAGES):
        halos = {}
        for way in (first, second):
            sent = edges[way].reshape(-1, lanes)
            halos[way] = lax.ppermute(sent, "gx", up if way == "up" else down).reshape(edge.shape)
        (sent,) = call(rows_kernel, [row_tile], [VMEM, VMEM], [state, phase_map], flops=cells * 10)
        before = lax.ppermute(sent.reshape(-1, lanes), "gy", over).reshape(sent.shape)
        after = before if across == 2 else lax.ppermute(sent, "gy", back)
        final = number == len(STAGES) - 1
        (state,) = call(
            functools.partial(middle_kernel, weights, number == 0),
            [whole],
            [VMEM] * 4,
            [coefs, state, phase_map, fields],
            flops=cells * 1000,
            scratch=[
                pltpu.VMEM((5, length + 2 * WIDTH, rows, lanes), jnp.float32),
                pltpu.VMEM((5, length, rows + 2 * TILE, lanes), jnp.float32),
                pltpu.VMEM((5, length, rows, lanes), jnp.float32),
            ],
        )
        state, *inner = call(
            functools.partial(border_kernel, weights[1], final),
            [whole, shaped(rows, lanes), whole] if final else [whole],
            [VMEM] * 5,
            [coefs, state, phase_map, before, after],
            flops=cells * 20,
            aliases={1: 0},
            places=[VMEM, VMEM, HBM] if final else None,
            scratch=[pltpu.SemaphoreType.DMA] if final else (),
        )
        if final:
            state, peak = call(
                functools.partial(final_kernel, weights[1]),
                [whole, shaped(along * across, lanes)],
                [VMEM] * 6,
                [coefs, state, halos["up"], halos["down"], phase_map, inner[0]],
                flops=cells * 50,
                aliases={1: 0},
            )
            break
        for way in STAGES[number + 1][0]:
            above = way == "up"
            state, edges[way] = call(
                functools.partial(join_kernel, weights[1], above),
                [whole, edge],
                [VMEM] * 4,
                [coefs, state, halos["down" if above else "up"], phase_map],
                flops=cells * 10,
                aliases={1: 0},
            )
    peaks = lax.all_to_all(peak, ("gx", "gy"), 0, 0, tiled=True)
    advanced, largest = call(
        output_kernel,
        [whole, shaped(1, lanes)],
        [VMEM, VMEM, HBM],
        [state, peaks, inner[1]],
        flops=1000,
        places=[HBM, HBM],
        scratch=[pltpu.VMEM((1, lanes), jnp.float32), pltpu.SemaphoreType.DMA((3,))],
        aliases={2: 0},
    )
    return (advanced, largest[0, 0:1])


def solution(mesh):
    return jax.shard_map(
        advance,
        mesh=mesh,
        in_specs=(P(None, "gx", "gy", None), P("gx", "gy", None), P(), P()),
        out_specs=(P(None, "gx", "gy", None), P()),
        check_vma=False,
    )
```
